16 devices in a mesh: dp: 2 (over y, z), fsdp: 8 (over x, core).
Axes of the slice: x: 4, y: 2, z: 1, core: 2. Of those that a mesh axis runs over, the one named last changes fastest.
The devices are a block of a 4x4x8 slice.
Arguments:
- hidden: bfloat16 [16, 1024, 2048], P(('dp', 'fsdp')), parts along dimension 0
- doc_lens: int32 [16], P(('dp', 'fsdp')), parts along dimension 0
- ln_par: float32 [2, 4, 2048], P(None, None, 'fsdp')
- w_qkv: bfloat16 [2, 2048, 8, 768], P(None, 'fsdp')
- b_qkv: bfloat16 [2, 6144], P(None, 'fsdp')
- w_out: bfloat16 [2, 2048, 2048], P(None, 'fsdp')
- b_out: bfloat16 [2, 2048], P(None, 'fsdp')
- w_up: bfloat16 [2, 2048, 8192], P(None, 'fsdp')
- b_up: bfloat16 [2, 8192], P(None, 'fsdp')
- w_down: bfloat16 [2, 8192, 2048], P(None, 'fsdp')
- b_down: bfloat16 [2, 2048], P(None, 'fsdp')
Outputs:
- output: bfloat16 [16, 1024, 2048], P(('dp', 'fsdp')), parts along dimension 0
There are 2 independent parts. The reference program is written for one: setup_inputs(seed, part) draws one part's arguments, and reference() takes and returns one part's arrays. A program takes and returns all parts, laid end to end along the dimension named above; an argument that names none is the same for every part.
All inputs are finite; a program needn't handle non-finite values.
Results may differ from the reference program's by a relative error of at most 0.0071295.
Values are sent between devices in bfloat16 or wider.
A program may use at most 768 MiB of HBM per device.

```python
import jax
import jax.numpy as jnp
from jax import lax

D_MODEL = 2048
NUM_HEADS = 8
HEAD_DIM = 256
FF_DIM = 8192
SEQ_LEN = 1024
NUM_DOCS = 8
NUM_LAYERS = 2
ROT_DIM = HEAD_DIM // 4
ROPE_BASE = 10000.0
LN_EPS = 1e-5


def setup_inputs(seed: int = 0, part: int = 0) -> dict:
    shared_key, doc_root = jax.random.split(jax.random.key(seed))
    part_key = jax.random.fold_in(doc_root, part)
    hidden_key, lens_key = jax.random.split(part_key)
    w_keys = jax.random.split(shared_key, 9)
    hidden = jax.random.normal(hidden_key, (NUM_DOCS, SEQ_LEN, D_MODEL), jnp.float32).astype(jnp.bfloat16)
    drawn_lens = jax.random.randint(lens_key, (NUM_DOCS,), 1, SEQ_LEN + 1, jnp.int32)
    doc_lens = drawn_lens.at[0].set(SEQ_LEN)
    ln_offset = jnp.array([1.0, 0.0, 1.0, 0.0], jnp.float32)[None, :, None]
    ln_par = ln_offset + 0.4 * jax.random.normal(w_keys[0], (NUM_LAYERS, 4, D_MODEL), jnp.float32)
    w_qkv = (jax.random.normal(w_keys[1], (NUM_LAYERS, D_MODEL, NUM_HEADS, 3 * HEAD_DIM), jnp.float32) * D_MODEL ** -0.5).astype(jnp.bfloat16)
    b_qkv = (0.5 * jax.random.normal(w_keys[2], (NUM_LAYERS, 3 * D_MODEL), jnp.float32)).astype(jnp.bfloat16)
    w_out = (jax.random.normal(w_keys[3], (NUM_LAYERS, D_MODEL, D_MODEL), jnp.float32) * D_MODEL ** -0.5).astype(jnp.bfloat16)
    b_out = (0.5 * jax.random.normal(w_keys[4], (NUM_LAYERS, D_MODEL), jnp.float32)).astype(jnp.bfloat16)
    w_up = (jax.random.normal(w_keys[5], (NUM_LAYERS, D_MODEL, FF_DIM), jnp.float32) * D_MODEL ** -0.5).astype(jnp.bfloat16)
    b_up = (0.5 * jax.random.normal(w_keys[6], (NUM_LAYERS, FF_DIM), jnp.float32)).astype(jnp.bfloat16)
    w_down = (jax.random.normal(w_keys[7], (NUM_LAYERS, FF_DIM, D_MODEL), jnp.float32) * FF_DIM ** -0.5).astype(jnp.bfloat16)
    b_down = (0.5 * jax.random.normal(w_keys[8], (NUM_LAYERS, D_MODEL), jnp.float32)).astype(jnp.bfloat16)
    return {'hidden': hidden, 'doc_lens': doc_lens, 'ln_par': ln_par, 'w_qkv': w_qkv, 'b_qkv': b_qkv, 'w_out': w_out, 'b_out': b_out, 'w_up': w_up, 'b_up': b_up, 'w_down': w_down, 'b_down': b_down}


def layer_norm(row_vals, gain_vec, shift_vec):
    mean_vals = jnp.mean(row_vals, axis=-1, keepdims=True)
    centered = row_vals - mean_vals
    var_vals = jnp.mean(centered * centered, axis=-1, keepdims=True)
    normed = centered * lax.rsqrt(var_vals + LN_EPS)
    return (normed * gain_vec + shift_vec).astype(jnp.bfloat16)


def rotary_tables(seq_len, rot_dim):
    inv_freq = 1.0 / (ROPE_BASE ** (jnp.arange(0, rot_dim, 2, dtype=jnp.float32) / rot_dim))
    angles = jnp.arange(seq_len, dtype=jnp.float32)[:, None] * inv_freq[None, :]
    angles = jnp.concatenate([angles, angles], axis=-1)
    return jnp.cos(angles), jnp.sin(angles)


def apply_rotary(head_vals, cos_tab, sin_tab):
    half_rot = ROT_DIM // 2
    rot_part = head_vals[..., :ROT_DIM].astype(jnp.float32)
    turned = jnp.concatenate([-rot_part[..., half_rot:], rot_part[..., :half_rot]], axis=-1)
    rotated = rot_part * cos_tab[:, None, :] + turned * sin_tab[:, None, :]
    return jnp.concatenate([rotated.astype(jnp.bfloat16), head_vals[..., ROT_DIM:]], axis=-1)


def doc_forward(doc_hidden, doc_len, layer_params, cos_tab, sin_tab):
    positions = jnp.arange(SEQ_LEN)
    visible = (positions[None, :] <= positions[:, None]) & (positions[None, :] < doc_len)

    def layer_step(x_cur, params):
        ln_rows, w_qkv_l, b_qkv_l, w_out_l, b_out_l, w_up_l, b_up_l, w_down_l, b_down_l = params
        x_rows = x_cur.astype(jnp.float32)
        attn_in = layer_norm(x_rows, ln_rows[0], ln_rows[1])
        mlp_in = layer_norm(x_rows, ln_rows[2], ln_rows[3])
        qkv_rows = jnp.dot(attn_in, w_qkv_l.reshape(D_MODEL, 3 * D_MODEL), preferred_element_type=jnp.float32) + b_qkv_l.astype(jnp.float32)
        qkv_heads = qkv_rows.astype(jnp.bfloat16).reshape(SEQ_LEN, NUM_HEADS, 3 * HEAD_DIM)
        queries = apply_rotary(qkv_heads[:, :, :HEAD_DIM], cos_tab, sin_tab)
        keys_rot = apply_rotary(qkv_heads[:, :, HEAD_DIM:2 * HEAD_DIM], cos_tab, sin_tab)
        values = qkv_heads[:, :, 2 * HEAD_DIM:]
        scores = jnp.einsum('qhe,khe->hqk', queries.astype(jnp.float32), keys_rot.astype(jnp.float32)) * (HEAD_DIM ** -0.5)
        prob_bf = jax.nn.softmax(jnp.where(visible[None], scores, -1e30), axis=-1).astype(jnp.bfloat16)
        context = jnp.einsum('hqk,khe->qhe', prob_bf.astype(jnp.float32), values.astype(jnp.float32))
        context = context.astype(jnp.bfloat16).reshape(SEQ_LEN, D_MODEL)
        attn_out = jnp.dot(context, w_out_l, preferred_element_type=jnp.float32) + b_out_l.astype(jnp.float32)
        up_rows = jnp.dot(mlp_in, w_up_l, preferred_element_type=jnp.float32) + b_up_l.astype(jnp.float32)
        act_rows = jax.nn.gelu(up_rows, approximate=False).astype(jnp.bfloat16)
        mlp_out = jnp.dot(act_rows, w_down_l, preferred_element_type=jnp.float32) + b_down_l.astype(jnp.float32)
        new_x = (x_rows + attn_out + mlp_out).astype(jnp.bfloat16)
        return new_x, None

    return lax.scan(layer_step, doc_hidden, layer_params)[0]


def reference(hidden, doc_lens, ln_par, w_qkv, b_qkv, w_out, b_out, w_up, b_up, w_down, b_down):
    cos_tab, sin_tab = rotary_tables(SEQ_LEN, ROT_DIM)
    layer_params = (ln_par, w_qkv, b_qkv, w_out, b_out, w_up, b_up, w_down, b_down)
    return lax.map(lambda doc_item: doc_forward(doc_item[0], doc_item[1], layer_params, cos_tab, sin_tab), (hidden, doc_lens))
```

```python
import functools

import jax
import jax.numpy as jnp
from jax import lax
from jax.experimental import pallas as pl
from jax.experimental.pallas import tpu as pltpu
from jax.sharding import PartitionSpec as P

ROPE_BASE = 10000.0
LN_EPS = 1e-5
MESH = pl.DeviceIdType.MESH
SLOTS = 16
LAG = 6
ROWS = 256
F32 = jnp.float32
BF16 = jnp.bfloat16


def rope_tables(seq_len, rot_dim, width):
    half = rot_dim // 2
    inv_freq = 1.0 / (ROPE_BASE ** (jnp.arange(0, rot_dim, 2, dtype=F32) / rot_dim))
    angles = jnp.arange(seq_len, dtype=F32)[:, None] * inv_freq[None, :]
    cos, sin = jnp.cos(angles), jnp.sin(angles)
    rest = width - rot_dim
    one, zero = jnp.ones((seq_len, rest), F32), jnp.zeros((seq_len, rest), F32)
    none = jnp.zeros((seq_len, half), F32)
    keep = jnp.concatenate([cos, cos, one], axis=1)
    low = jnp.concatenate([-sin, none, zero], axis=1)
    high = jnp.concatenate([none, sin, zero], axis=1)
    return jnp.stack([keep, low, high])


def kernel(dims, hid, lens, small, tabs, wq, wo, wu, wd, out, gath, xs, a_s, m_s, ctx, act, acc, q_s, k_s, v_s, wbuf,
           smallg, send, cw, ccw, ysem, dd, ld, small_send, small_recv, io_sem):
    n, num_layers, heads, tile, seq, d_model, rps, rot_half = dims
    ring = n // 2
    n_a, n_b, n_c = heads, n * rps // 2, d_model // tile
    per_layer = n_a + n_b + n_c
    chunks = num_layers * per_layer
    wide = tabs.shape[2]
    scale = float(tile) ** -0.5

    d, f = lax.axis_index("dp"), lax.axis_index("fsdp")
    x, c = f // 2, f % 2
    par = d % 2
    right = ((x + 1) % ring) * 2 + c
    left = ((x + ring - 1) % ring) * 2 + c
    sib = x * 2 + 1 - c
    mate = d + 1 - 2 * par
    mine, other = 2 * par, 2 - 2 * par

    def remote(src, dst, s_sem, r_sem, where):
        return pltpu.make_async_remote_copy(
            src_ref=src, dst_ref=dst, send_sem=s_sem, recv_sem=r_sem, device_id=where, device_id_type=MESH)

    to_right, to_left, to_sib, to_mate = {"fsdp": right}, {"fsdp": left}, {"fsdp": sib}, {"dp": mate}

    def q_tile(l, r, i):
        return wq.at[l, :, pl.ds(pl.multiple_of(r * (3 * tile) + i * tile, tile), tile)]

    def up_tile(l, u):
        return wu.at[l, :, pl.ds(pl.multiple_of((u % n) * (rps * tile) + (u // n) * tile, tile), tile)]

    def down_tile(l, v):
        return wd.at[l, pl.ds(pl.multiple_of((v // n_c) * tile, tile), tile),
                     pl.ds(pl.multiple_of((v % n_c) * tile, tile), tile)]

    def out_tile(l, j):
        return wo.at[l, :, pl.ds(pl.multiple_of(j * tile, tile), tile)]

    def send_own(k):
        slot = k % SLOTS
        l, r = k // per_layer, k % per_layer

        def go(own):
            remote(own(mine), gath.at[k, mine, f], send.at[slot], cw.at[slot, 0], to_right).start()
            remote(own(1), gath.at[k, 1, f], send.at[slot], ccw.at[slot, 0], to_left).start()
            for i in range(3):
                remote(own(i), gath.at[k, i, f], send.at[slot], dd.at[slot], to_sib).start()

        @pl.when(r < n_a)
        def _():
            go(lambda i: q_tile(l, r, i))

        @pl.when((r >= n_a) & (r < n_a + n_b))
        def _():
            j = r - n_a
            go(lambda i: down_tile(l, j) if isinstance(i, int) and i == 1 else up_tile(l, 2 * j + i // 2))

        @pl.when(r >= n_a + n_b)
        def _():
            j = r - n_a - n_b
            go(lambda i: out_tile(l, j) if isinstance(i, int) and i == 1 else down_tile(l, n_b + 2 * j + i // 2))

    def from_left(hop):
        return ((x + ring - hop) % ring) * 2 + c

    def from_right(hop):
        return ((x + hop) % ring) * 2 + c

    def wait_tile(sem):
        ref = gath.at[0, 0, 0]
        pltpu.make_async_copy(ref, ref, sem).wait()

    def pass_on(k, hop):
        slot = k % SLOTS
        fx, fy = from_left(hop), from_right(hop)
        wait_tile(cw.at[slot, hop - 1])
        t_cw = gath.at[k, mine, fx]
        if hop < ring - 1:
            remote(t_cw, t_cw, send.at[slot], cw.at[slot, hop], to_right).start()
        remote(t_cw, t_cw, send.at[slot], ysem.at[slot, hop - 1], to_mate).start()
        remote(t_cw, t_cw, send.at[slot], dd.at[slot], to_sib).start()
        wait_tile(ccw.at[slot, hop - 1])
        t_ccw = gath.at[k, 1, fy]
        if hop < ring - 1:
            remote(t_ccw, t_ccw, send.at[slot], ccw.at[slot, hop], to_left).start()
        remote(t_ccw, t_ccw, send.at[slot], dd.at[slot], to_sib).start()

    def pass_mate(k, hop):
        slot = k % SLOTS
        wait_tile(ysem.at[slot, hop - 1])
        t_y = gath.at[k, other, from_left(hop)]
        remote(t_y, t_y, send.at[slot], dd.at[slot], to_sib).start()

    sib_tiles = 3 * ring
    sent_tiles = 2 * (ring - 1) + (ring - 1) + sib_tiles

    def wait_sib(k):
        ref = gath.at[0, :, pl.ds(0, sib_tiles // 3)]
        pltpu.make_async_copy(ref, ref, dd.at[k % SLOTS]).wait()

    def wait_sent(k):
        ref = gath.at[0, :, pl.ds(0, sent_tiles // 3)]
        pltpu.make_async_copy(ref, ref, send.at[k % SLOTS]).wait()

    def load_tile(k, i, to, own):
        slot = k % 2
        kk = k if to < 3 else k - 4
        for step in range(1, n):
            s = (f + step) % n
            pltpu.make_async_copy(
                gath.at[kk, i, s], wbuf.at[slot, to, pl.ds(pl.multiple_of(s * tile, tile), tile)], ld.at[slot, to]).start()
        pltpu.make_async_copy(own, wbuf.at[slot, to, pl.ds(pl.multiple_of(f * tile, tile), tile)], ld.at[slot, to]).start()

    def load(k):
        l, r = k // per_layer, k % per_layer

        @pl.when(r < n_a)
        def _():
            for i in range(3):
                load_tile(k, i, i, q_tile(l, r, i))

        @pl.when((r >= n_a) & (r < n_a + n_b))
        def _():
            for i in (0, 2):
                load_tile(k, i, i, up_tile(l, 2 * (r - n_a) + i // 2))

        @pl.when(r >= n_a + n_b)
        def _():
            j = r - n_a - n_b
            load_tile(k, 0, 0, down_tile(l, n_b + 2 * j))
            load_tile(k, 1, 1, out_tile(l, j))
            load_tile(k, 2, 2, down_tile(l, n_b + 2 * j + 1))

        @pl.when((r >= n_a + 4) & (r < n_a + n_b + 4))
        def _():
            load_tile(k, 1, 3, down_tile(l, r - n_a - 4))

    def loaded(slot, to):
        pltpu.make_async_copy(wbuf.at[slot, to], wbuf.at[slot, to], ld.at[slot, to]).wait()

    def within(k, do):
        @pl.when((k >= 0) & (k < chunks))
        def _():
            do(k)

    def sub0(t):
        within(t - 8, wait_sent)
        within(t, send_own)
        within(t - 4, lambda k: pass_on(k, 3))
        within(t - 4, lambda k: pass_mate(k, 2))

    def sub1(t):
        within(t - 1, lambda k: pass_on(k, 1))
        within(t - 5, lambda k: pass_mate(k, 3))

    def sub2(t):
        within(t - 2, lambda k: pass_on(k, 2))
        within(t - 2, lambda k: pass_mate(k, 1))
        within(t - 5, wait_sib)
        within(t - 5, load)

    blocks = seq // ROWS

    def rows_of(b):
        return pl.ds(b * ROWS, ROWS)

    def cols_of(j):
        return pl.ds(pl.multiple_of(j * tile, tile), tile)

    def row(s, l, i):
        return smallg[s, l, pl.ds(i, 1), :]

    def layer_norms(l):
        step = 128

        def body(b, carry):
            rows = pl.ds(pl.multiple_of(b * step, step), step)
            v = xs[rows, :].astype(F32)
            cen = v - jnp.mean(v, axis=-1, keepdims=True)
            inv = lax.rsqrt(jnp.mean(cen * cen, axis=-1, keepdims=True) + LN_EPS)
            for s in range(n):
                cols = pl.ds(s * tile, tile)
                norm = cen[:, s * tile:(s + 1) * tile] * inv
                a_s[rows, cols] = (norm * row(s, l, 0) + row(s, l, 1)).astype(BF16)
                m_s[rows, cols] = (norm * row(s, l, 2) + row(s, l, 3)).astype(BF16)
                acc[rows, cols] = v[:, s * tile:(s + 1) * tile] + (row(s, l, 7) + row(s, l, 8 + rps))
            return carry

        lax.fori_loop(0, seq // step, body, 0)

    def dot(lhs, slot, to):
        return jnp.dot(lhs, wbuf[slot, to], preferred_element_type=F32)

    def rotate(v, rows):
        u = v[:, :wide].astype(F32)
        turned = (u * tabs[0, rows, :] + pltpu.roll(u, wide - rot_half, 1) * tabs[1, rows, :]
                  + pltpu.roll(u, rot_half, 1) * tabs[2, rows, :])
        return turned.astype(BF16)

    def project(l, h, slot, i, ref):
        for b in range(blocks):
            v = (dot(a_s[rows_of(b), :], slot, i) + row(h, l, 4 + i)).astype(BF16)
            if i < 2:
                ref[rows_of(b), pl.ds(0, wide)] = rotate(v, rows_of(b))
                ref[rows_of(b), pl.ds(wide, tile - wide)] = v[:, wide:]
            else:
                ref[rows_of(b), :] = v

    def attend(h, b):
        width = (b + 1) * ROWS
        s = lax.dot_general(q_s[rows_of(b), :], k_s[pl.ds(0, width), :], (((1,), (1,)), ((), ())),
                            preferred_element_type=F32) * scale
        col = lax.broadcasted_iota(jnp.int32, (ROWS, width), 1)
        at = lax.broadcasted_iota(jnp.int32, (ROWS, width), 0) + b * ROWS
        s = jnp.where((col <= at) & (col < lens[0:1, 0:1]), s, -1e30)
        e = jnp.exp(s - jnp.max(s, axis=-1, keepdims=True))
        p = (e * (1.0 / jnp.sum(e, axis=-1, keepdims=True))).astype(BF16)
        ctx[rows_of(b), cols_of(h)] = jnp.dot(p, v_s[pl.ds(0, width), :], preferred_element_type=F32).astype(BF16)

    def up(l, u, slot, to):
        s, rp = u % n, u // n
        for b in range(blocks):
            v = dot(m_s[rows_of(b), :], slot, to) + row(s, l, 8 + rp)
            g = (0.5 * v) * (1.0 + lax.erf(v * (0.5 ** 0.5)))
            act[rp, rows_of(b), cols_of(s)] = g.astype(BF16)

    def add_to(j, slot, to, lhs):
        for b in range(blocks):
            acc[rows_of(b), cols_of(j)] += dot(lhs(rows_of(b)), slot, to)

    def down(v, slot, to):
        add_to(v % n_c, slot, to, lambda rows: act[v // n_c, rows, :])

    def head_step(l, h):
        k = l * per_layer + h
        t, slot = k + LAG, k % 2
        sub0(t)
        for i in range(3):
            loaded(slot, i)
        project(l, h, slot, 0, q_s)
        project(l, h, slot, 1, k_s)
        sub1(t)
        project(l, h, slot, 2, v_s)
        for b in range(blocks // 2):
            attend(h, b)
        sub2(t)
        for b in range(blocks // 2, blocks):
            attend(h, b)

    def up_step(l, j):
        k = l * per_layer + n_a + j
        t, slot = k + LAG, k % 2
        sub0(t)
        loaded(slot, 0)
        up(l, 2 * j, slot, 0)
        sub1(t)
        loaded(slot, 2)
        up(l, 2 * j + 1, slot, 2)
        sub2(t)

        @pl.when(j >= 4)
        def _():
            loaded(slot, 3)
            down(j - 4, slot, 3)

    def down_step(l, j):
        k = l * per_layer + n_a + n_b + j
        t, slot = k + LAG, k % 2
        sub0(t)
        loaded(slot, 0)
        down(n_b + 2 * j, slot, 0)
        sub1(t)
        loaded(slot, 2)
        down(n_b + 2 * j + 1, slot, 2)
        sub2(t)
        loaded(slot, 1)
        add_to(j, slot, 1, lambda rows: ctx[rows, :])

        @pl.when(j < 4)
        def _():
            loaded(slot, 3)
            down(n_b - 4 + j, slot, 3)

    get_hidden = pltpu.make_async_copy(hid, xs, io_sem)
    get_hidden.start()
    barrier = pltpu.get_barrier_semaphore()
    for step in range(1, n):
        pl.semaphore_signal(barrier, inc=1, device_id={"fsdp": (f + step) % n}, device_id_type=MESH)
    pl.semaphore_signal(barrier, inc=1, device_id=to_mate, device_id_type=MESH)
    pl.semaphore_wait(barrier, n)

    sub0(0)
    smalls = [
        remote(small, smallg.at[f], small_send.at[step - 1], small_recv.at[step - 1], {"fsdp": (f + step) % n})
        for step in range(1, n)
    ]
    for copy in smalls:
        copy.start()
    smallg[f] = small[...]
    sub0(1)
    sub1(1)
    for copy in smalls:
        copy.wait()
    get_hidden.wait()
    layer_norms(0)
    sub2(1)

    def fill(t, carry):
        sub0(t)
        sub1(t)
        sub2(t)
        return carry

    lax.fori_loop(2, LAG, fill, 0)

    def layer(l, carry):
        def loop(count, step):
            def body(i, inner):
                step(l, i)
                return inner

            lax.fori_loop(0, count, body, 0)

        @pl.when(l > 0)
        def _():
            layer_norms(l)

        loop(n_a, head_step)
        loop(n_b, up_step)
        loop(n_c, down_step)
        for b in range(blocks):
            xs[rows_of(b), :] = acc[rows_of(b), :].astype(BF16)
        return carry

    lax.fori_loop(0, num_layers, layer, 0)
    put = pltpu.make_async_copy(xs, out, io_sem)
    put.start()
    wait_sent(chunks - 2)
    wait_sent(chunks - 1)
    put.wait()


def solution(mesh):
    row_spec = P(("dp", "fsdp"), None, None)
    in_specs = (row_spec, P(("dp", "fsdp")), P(None, None, "fsdp"), P(None, "fsdp", None, None), P(None, "fsdp"),
                P(None, "fsdp", None), P(None, "fsdp"), P(None, "fsdp", None), P(None, "fsdp"), P(None, "fsdp", None),
                P(None, "fsdp"))
    n = mesh.shape["fsdp"]
    assert n % 2 == 0 and mesh.shape["dp"] % 2 == 0

    def local_step(hidden, lens, ln_par, w_qkv, b_qkv, w_out, b_out, w_up, b_up, w_down, b_down):
        _, seq, d_model = hidden.shape
        num_layers, tile, heads, triple = w_qkv.shape
        rps = w_down.shape[1] // tile
        assert hidden.shape[0] == 1 and n * tile == d_model and triple == 3 * tile and heads == n
        assert n * rps // 2 + 2 * (d_model // tile) == n * rps
        rot_half = tile // 8
        wide = 128
        per = [(num_layers, -1, tile)] * 4
        small = jnp.concatenate(
            [ln_par] + [b.astype(F32).reshape(p) for b, p in zip((b_qkv, b_out, b_up, b_down), per)], axis=1)
        small = jnp.pad(small, ((0, 0), (0, -small.shape[1] % 8), (0, 0)))
        tabs = rope_tables(seq, 2 * rot_half, wide)
        dims = (n, num_layers, heads, tile, seq, d_model, rps, rot_half)
        chunks = num_layers * (heads + n * rps // 2 + d_model // tile)
        ring = n // 2
        vmem = pl.BlockSpec(memory_space=pltpu.VMEM)
        anywhere = pl.BlockSpec(memory_space=pl.ANY)
        dma = pltpu.SemaphoreType.DMA
        out, _ = pl.pallas_call(
            functools.partial(kernel, dims),
            name="layers",
            out_shape=(jax.ShapeDtypeStruct((seq, d_model), BF16),
                       jax.ShapeDtypeStruct((chunks, 3, n, tile, tile), BF16)),
            in_specs=[anywhere, vmem, vmem, vmem] + [anywhere] * 4,
            out_specs=(anywhere, anywhere),
            scratch_shapes=[
                pltpu.VMEM((seq, d_model), BF16),
                pltpu.VMEM((seq, d_model), BF16),
                pltpu.VMEM((seq, d_model), BF16),
                pltpu.VMEM((seq, d_model), BF16),
                pltpu.VMEM((rps, seq, d_model), BF16),
                pltpu.VMEM((seq, d_model), F32),
                pltpu.VMEM((seq, tile), BF16),
                pltpu.VMEM((seq, tile), BF16),
                pltpu.VMEM((seq, tile), BF16),
                pltpu.VMEM((2, 4, d_model, tile), BF16),
                pltpu.VMEM((n,) + small.shape, F32),
                dma((SLOTS,)),
                dma((SLOTS, ring - 1)),
                dma((SLOTS, ring - 1)),
                dma((SLOTS, ring - 1)),
                dma((SLOTS,)),
                dma((2, 4)),
                dma((n - 1,)),
                dma((n - 1,)),
                dma,
            ],
            compiler_params=pltpu.CompilerParams(
                collective_id=0, has_side_effects=True, vmem_limit_bytes=67043328),
        )(hidden.reshape(seq, d_model), jnp.broadcast_to(lens.reshape(1, 1), (8, 128)), small, tabs,
          w_qkv.reshape(num_layers, tile, heads * triple), w_out, w_up, w_down)
        return out.reshape(1, seq, d_model)

    return jax.shard_map(local_step, mesh=mesh, in_specs=in_specs, out_specs=row_spec, check_vma=False)
```

```python
import functools

import jax
import jax.numpy as jnp
import numpy as np
from jax import lax
from jax.experimental import pallas as pl
from jax.experimental.pallas import tpu as pltpu
from jax.sharding import PartitionSpec as P

ROPE_BASE = 10000.0
LN_EPS = 1e-5
MESH = pl.DeviceIdType.MESH
SLOTS = 16
LATE = 4
ROWS = 256
F32 = jnp.float32
BF16 = jnp.bfloat16


def rope_row(rot_dim, width):
    inv_freq = np.float32(1.0) / (np.float32(ROPE_BASE) ** (np.arange(0, rot_dim, 2, dtype=np.float32) / np.float32(rot_dim)))
    row = np.concatenate([inv_freq, inv_freq, np.zeros(width - rot_dim, np.float32)])
    return np.broadcast_to(row.astype(np.float32), (8, width))


def kernel(dims, hid, lens, freq, ln_own, bq_own, bo_own, bu_own, bd_own, wq_raw, wo, wu, wd, out, gath, wq, xs, a_s, m_s, ctx,
           act, acc, q_s, k_s, v_s, wbuf, tabs, ln_g, bq_g, bo_g, bu_g, bd_g, bias, raw, raw32, turned, send, rs, ls, ysem, dd,
           ld, small_send, small_recv, raw_in, raw_out, io_sem):
    n, num_layers, heads, tile, seq, d_model, rps, rot_half = dims
    ring = n // 2
    n_a, n_b, n_c = heads, n * rps // 2, d_model // tile
    per_layer = n_a + n_b + n_c
    chunks = num_layers * per_layer
    wide = tabs.shape[2]
    scale = float(tile) ** -0.5

    d, f = lax.axis_index("dp"), lax.axis_index("fsdp")
    x, c = f // 2, f % 2
    par = d % 2
    right = ((x + 1) % ring) * 2 + c
    left = ((x + ring - 1) % ring) * 2 + c
    far = ((x + 2) % ring) * 2 + c
    sib = x * 2 + 1 - c
    mate = d + 1 - 2 * par
    mine, other = 2 * par, 2 - 2 * par

    def remote(src, dst, s_sem, r_sem, where):
        return pltpu.make_async_remote_copy(
            src_ref=src, dst_ref=dst, send_sem=s_sem, recv_sem=r_sem, device_id=where, device_id_type=MESH)

    to_right, to_left, to_sib, to_mate = {"fsdp": right}, {"fsdp": left}, {"fsdp": sib}, {"dp": mate}

    def q_tile(l, h, i):
        return wq.at[l, h, :, pl.ds(i * tile, tile) if isinstance(i, int) else pl.ds(pl.multiple_of(i * tile, tile), tile)]

    def up_tile(l, u):
        return wu.at[l, :, pl.ds(pl.multiple_of((u % n) * (rps * tile) + (u // n) * tile, tile), tile)]

    def down_tile(l, v):
        return wd.at[l, pl.ds(pl.multiple_of((v // n_c) * tile, tile), tile),
                     pl.ds(pl.multiple_of((v % n_c) * tile, tile), tile)]

    def out_tile(l, j):
        return wo.at[l, :, pl.ds(pl.multiple_of(j * tile, tile), tile)]

    def with_own(k, go):
        l, r = k // per_layer, k % per_layer

        @pl.when(r < n_b)
        def _():
            go(lambda i: down_tile(l, r) if isinstance(i, int) and i == 1 else up_tile(l, 2 * r + i // 2))

        @pl.when((r >= n_b) & (r < n_b + n_a))
        def _():
            go(lambda i: q_tile(l, r - n_b, i))

        @pl.when(r >= n_a + n_b)
        def _():
            j = r - n_a - n_b
            go(lambda i: out_tile(l, j) if isinstance(i, int) and i == 1 else down_tile(l, n_b + 2 * j + i // 2))

    def own_first(k):
        slot = k % SLOTS

        def go(own):
            remote(own(mine), gath.at[k, mine, f], send.at[slot], rs.at[slot, 0], to_right).start()
            remote(own(1), gath.at[k, 1, f], send.at[slot], ls.at[slot, 0], to_left).start()
            for i in (mine, 1):
                remote(own(i), gath.at[k, i, f], send.at[slot], dd.at[slot], to_sib).start()

        with_own(k, go)

    def own_second(k):
        slot = k % SLOTS

        def go(own):
            remote(own(1), gath.at[k, 1, f], send.at[slot], rs.at[slot, 1], to_right).start()
            remote(own(mine), gath.at[k, mine, f], send.at[slot], ls.at[slot, 1], to_left).start()
            remote(own(other), gath.at[k, other, f], send.at[slot], dd.at[slot], to_sib).start()

        with_own(k, go)

    def wait_tile(sem):
        ref = gath.at[0, 0, 0]
        pltpu.make_async_copy(ref, ref, sem).wait()

    def pass_on(k, i, s, sem, where):
        t = gath.at[k, i, s]
        remote(t, t, send.at[k % SLOTS], sem, where).start()

    def from_sides(k):
        slot = k % SLOTS
        wait_tile(rs.at[slot, 0])
        pass_on(k, mine, left, rs.at[slot, 2], to_right)
        pass_on(k, mine, left, ysem.at[slot, 0], to_mate)
        pass_on(k, mine, left, dd.at[slot], to_sib)
        wait_tile(ls.at[slot, 0])
        pass_on(k, 1, right, ls.at[slot, 2], to_left)
        pass_on(k, 1, right, dd.at[slot], to_sib)

    def from_sides_again(k):
        slot = k % SLOTS
        wait_tile(ls.at[slot, 1])
        pass_on(k, mine, right, ysem.at[slot, 1], to_mate)
        pass_on(k, mine, right, dd.at[slot], to_sib)
        wait_tile(rs.at[slot, 1])
        pass_on(k, 1, left, dd.at[slot], to_sib)

    def from_far(k):
        slot = k % SLOTS
        wait_tile(rs.at[slot, 2])
        pass_on(k, mine, far, ysem.at[slot, 2], to_mate)
        pass_on(k, mine, far, dd.at[slot], to_sib)
        wait_tile(ls.at[slot, 2])
        pass_on(k, 1, far, dd.at[slot], to_sib)

    def from_mate(i, s):
        def do(k):
            slot = k % SLOTS
            wait_tile(ysem.at[slot, i])
            pass_on(k, other, s, dd.at[slot], to_sib)

        return do

    sib_tiles = 3 * ring
    sent_tiles = 3 * (ring - 1) + sib_tiles

    def wait_sib(k):
        ref = gath.at[0, :, pl.ds(0, sib_tiles // 3)]
        pltpu.make_async_copy(ref, ref, dd.at[k % SLOTS]).wait()

    def wait_sent(k):
        ref = gath.at[0, :, pl.ds(0, sent_tiles // 3)]
        pltpu.make_async_copy(ref, ref, send.at[k % SLOTS]).wait()

    def load_tile(k, kk, i, to, own):
        slot = k % 2
        for step in range(1, n):
            s = (f + step) % n
            pltpu.make_async_copy(
                gath.at[kk, i, s], wbuf.at[slot, to, pl.ds(pl.multiple_of(s * tile, tile), tile)], ld.at[slot, to]).start()
        pltpu.make_async_copy(own, wbuf.at[slot, to, pl.ds(pl.multiple_of(f * tile, tile), tile)], ld.at[slot, to]).start()

    def load(k):
        l, r = k // per_layer, k % per_layer
        j = r - n_a - n_b

        @pl.when(r < n_b)
        def _():
            for i in (0, 2):
                load_tile(k, k, i, i, up_tile(l, 2 * r + i // 2))

        @pl.when((r >= LATE) & (r < n_b))
        def _():
            load_tile(k, k - LATE, 1, 3, down_tile(l, r - LATE))

        @pl.when((r >= n_b) & (r < n_b + n_a))
        def _():
            for i in range(3):
                load_tile(k, k, i, i, q_tile(l, r - n_b, i))

        @pl.when(r >= n_a + n_b)
        def _():
            load_tile(k, k, 0, 0, down_tile(l, n_b + 2 * j))
            load_tile(k, k, 1, 1, out_tile(l, j))
            load_tile(k, k, 2, 2, down_tile(l, n_b + 2 * j + 1))

        @pl.when((r >= n_a + n_b) & (j < LATE))
        def _():
            load_tile(k, k - n_a - LATE, 1, 3, down_tile(l, n_b - LATE + j))

    def loaded(slot, to):
        pltpu.make_async_copy(wbuf.at[slot, to], wbuf.at[slot, to], ld.at[slot, to]).wait()

    def within(k, do):
        @pl.when((k >= 0) & (k < chunks))
        def _():
            do(k)

    def part0(t):
        within(t - 7, wait_sent)
        within(t, own_first)
        within(t - 2, from_sides_again)
        within(t - 4, wait_sib)
        within(t - 4, load)

    def part1(t):
        within(t - 1, from_sides)
        within(t - 3, from_mate(1, right))

    def part2(t):
        within(t, own_second)
        within(t - 2, from_far)
        within(t - 2, from_mate(0, left))
        within(t - 3, from_mate(2, far))

    blocks = seq // ROWS

    def rows_of(b):
        return pl.ds(b * ROWS, ROWS)

    def cols_of(j):
        return pl.ds(pl.multiple_of(j * tile, tile), tile)

    def row(s, l, i):
        return bias[s, l, pl.ds(i, 1), :]

    def ln_row(s, l, i):
        return ln_g[s, l, pl.ds(i, 1), :]

    def layer_norms(l):
        step = 128

        def body(b, carry):
            rows = pl.ds(pl.multiple_of(b * step, step), step)
            v = xs[rows, :].astype(F32)
            cen = v - jnp.mean(v, axis=-1, keepdims=True)
            inv = lax.rsqrt(jnp.mean(cen * cen, axis=-1, keepdims=True) + LN_EPS)
            for s in range(n):
                cols = pl.ds(s * tile, tile)
                norm = cen[:, s * tile:(s + 1) * tile] * inv
                a_s[rows, cols] = (norm * ln_row(s, l, 0) + ln_row(s, l, 1)).astype(BF16)
                m_s[rows, cols] = (norm * ln_row(s, l, 2) + ln_row(s, l, 3)).astype(BF16)
                acc[rows, cols] = v[:, s * tile:(s + 1) * tile] + (row(s, l, 3) + row(s, l, 4 + rps))
            return carry

        lax.fori_loop(0, seq // step, body, 0)

    def dot(lhs, slot, to):
        return jnp.dot(lhs, wbuf[slot, to], preferred_element_type=F32)

    def rotate(v, rows):
        u = v[:, :wide].astype(F32)
        turned = (u * tabs[0, rows, :] + pltpu.roll(u, wide - rot_half, 1) * tabs[1, rows, :]
                  + pltpu.roll(u, rot_half, 1) * tabs[2, rows, :])
        return turned.astype(BF16)

    def project(l, h, slot, i, ref):
        for b in range(blocks):
            v = (dot(a_s[rows_of(b), :], slot, i) + row(h, l, i)).astype(BF16)
            if i < 2:
                ref[rows_of(b), pl.ds(0, wide)] = rotate(v, rows_of(b))
                ref[rows_of(b), pl.ds(wide, tile - wide)] = v[:, wide:]
            else:
                ref[rows_of(b), :] = v

    def attend(h, b):
        width = (b + 1) * ROWS
        s = lax.dot_general(q_s[rows_of(b), :], k_s[pl.ds(0, width), :], (((1,), (1,)), ((), ())),
                            preferred_element_type=F32) * scale
        col = lax.broadcasted_iota(jnp.int32, (ROWS, width), 1)
        at = lax.broadcasted_iota(jnp.int32, (ROWS, width), 0) + b * ROWS
        s = jnp.where((col <= at) & (col < lens[0]), s, -1e30)
        e = jnp.exp(s - jnp.max(s, axis=-1, keepdims=True))
        p = (e * (1.0 / jnp.sum(e, axis=-1, keepdims=True))).astype(BF16)
        ctx[rows_of(b), cols_of(h)] = jnp.dot(p, v_s[pl.ds(0, width), :], preferred_element_type=F32).astype(BF16)

    def up(l, u, slot, to):
        s, rp = u % n, u // n
        for b in range(blocks):
            v = dot(m_s[rows_of(b), :], slot, to) + row(s, l, 4 + rp)
            g = (0.5 * v) * (1.0 + lax.erf(v * (0.5 ** 0.5)))
            act[rp, rows_of(b), cols_of(s)] = g.astype(BF16)

    def add_to(j, slot, to, lhs):
        for b in range(blocks):
            acc[rows_of(b), cols_of(j)] += dot(lhs(rows_of(b)), slot, to)

    def down(v, slot, to):
        add_to(v % n_c, slot, to, lambda rows: act[v // n_c, rows, :])

    def head_step(l, h):
        k = l * per_layer + n_b + h
        slot = k % 2
        part1(k + 4)
        loaded(slot, 0)
        loaded(slot, 1)
        project(l, h, slot, 0, q_s)
        project(l, h, slot, 1, k_s)
        part2(k + 4)
        loaded(slot, 2)
        project(l, h, slot, 2, v_s)
        for b in range(blocks // 2):
            attend(h, b)
        part0(k + 5)
        for b in range(blocks // 2, blocks):
            attend(h, b)

    def up_step(l, j):
        k = l * per_layer + j
        slot = k % 2
        part1(k + 4)
        loaded(slot, 0)
        up(l, 2 * j, slot, 0)
        part2(k + 4)
        loaded(slot, 2)
        up(l, 2 * j + 1, slot, 2)
        part0(k + 5)

        @pl.when(j >= LATE)
        def _():
            loaded(slot, 3)
            down(j - LATE, slot, 3)

    def down_step(l, j):
        k = l * per_layer + n_a + n_b + j
        slot = k % 2
        part1(k + 4)
        loaded(slot, 0)
        down(n_b + 2 * j, slot, 0)

        @pl.when(j < LATE)
        def _():
            loaded(slot, 3)
            down(n_b - LATE + j, slot, 3)

        part2(k + 4)
        loaded(slot, 2)
        down(n_b + 2 * j + 1, slot, 2)
        part0(k + 5)
        loaded(slot, 1)
        add_to(j, slot, 1, lambda rows: ctx[rows, :])

    def rotary_tables():
        for b in range(blocks):
            at = (lax.broadcasted_iota(jnp.int32, (ROWS, wide), 0) + b * ROWS).astype(F32)
            lane = lax.broadcasted_iota(jnp.int32, (ROWS, wide), 1)
            angle = at * freq[0:1, :]
            cos, sin = jnp.cos(angle), jnp.sin(angle)
            tabs[0, rows_of(b), :] = jnp.where(lane < 2 * rot_half, cos, 1.0)
            tabs[1, rows_of(b), :] = jnp.where(lane < rot_half, -sin, 0.0)
            tabs[2, rows_of(b), :] = jnp.where((lane >= rot_half) & (lane < 2 * rot_half), sin, 0.0)

    raw_rows = raw.shape[1]
    per_raw = tile * heads // raw_rows
    raws = num_layers * per_raw

    def get_raw(b):
        return pltpu.make_async_copy(
            wq_raw.at[b // per_raw, pl.ds(pl.multiple_of((b % per_raw) * raw_rows, raw_rows), raw_rows)],
            raw.at[b % 2], raw_in.at[b % 2])

    def put_raw(b):
        some = raw_rows // heads
        return pltpu.make_async_copy(
            turned.at[b % 2], wq.at[b // per_raw, :, pl.ds(pl.multiple_of((b % per_raw) * some, some), some)],
            raw_out.at[b % 2])

    def by_head(first, last):
        def body(b, carry):
            get_raw(b).wait()
            for q in range(raw.shape[2] // wide):
                raw32[pl.ds(q * raw_rows, raw_rows), :] = raw[b % 2, :, pl.ds(q * wide, wide)].astype(F32)

            @pl.when(b + 2 < raws)
            def _():
                get_raw(b + 2).start()

            @pl.when(b >= 2)
            def _():
                put_raw(b - 2).wait()

            for h in range(heads):
                for q in range(raw.shape[2] // wide):
                    turned[b % 2, h, :, pl.ds(q * wide, wide)] = (
                        raw32[pl.ds(q * raw_rows + h, raw_rows // heads, stride=heads), :].astype(BF16))
            put_raw(b).start()
            return carry

        lax.fori_loop(first, last, body, 0)

    def unpack_biases():
        for s in range(n):
            for g, at, count in ((bq_g, 0, 3), (bo_g, 3, 1), (bu_g, 4, rps), (bd_g, 4 + rps, 1)):
                for i in range(count):
                    v = g[s, :, pl.ds(i * tile, tile)].astype(F32)
                    for l in range(num_layers):
                        bias[s, l, pl.ds(at + i, 1), :] = v[l:l + 1]

    get_hidden = pltpu.make_async_copy(hid, xs, io_sem)
    get_hidden.start()
    get_raw(0).start()
    get_raw(1).start()
    barrier = pltpu.get_barrier_semaphore()
    for step in range(1, n):
        pl.semaphore_signal(barrier, inc=1, device_id={"fsdp": (f + step) % n}, device_id_type=MESH)
    pl.semaphore_signal(barrier, inc=1, device_id=to_mate, device_id_type=MESH)
    pl.semaphore_wait(barrier, n)

    own_first(0)
    own_second(0)
    part0(1)
    smalls = ((ln_own, ln_g), (bq_own, bq_g), (bo_own, bo_g), (bu_own, bu_g), (bd_own, bd_g))
    for i, (own, everyone) in enumerate(smalls):
        for step in range(1, n):
            remote(own, everyone.at[f], small_send.at[i], small_recv.at[i], {"fsdp": (f + step) % n}).start()
        everyone[f] = own[...]
    rotary_tables()
    part1(1)
    for i, (own, everyone) in enumerate(smalls):
        ref = everyone.at[pl.ds(0, n - 1)]
        pltpu.make_async_copy(ref, ref, small_send.at[i]).wait()
        pltpu.make_async_copy(ref, ref, small_recv.at[i]).wait()
    unpack_biases()
    part2(1)
    get_hidden.wait()
    layer_norms(0)
    cuts = [raws * i // 6 for i in range(7)]
    for i, (part, t) in enumerate(((part0, 2), (part1, 2), (part2, 2), (part0, 3), (part1, 3), (part2, 3))):
        part(t)
        by_head(cuts[i], cuts[i + 1])
    put_raw(raws - 2).wait()
    put_raw(raws - 1).wait()
    part0(4)

    def layer(l, carry):
        def loop(count, step):
            def body(i, inner):
                step(l, i)
                return inner

            lax.fori_loop(0, count, body, 0)

        @pl.when(l > 0)
        def _():
            layer_norms(l)

        loop(n_b, up_step)
        loop(n_a, head_step)
        loop(n_c, down_step)
        for b in range(blocks):
            xs[rows_of(b), :] = acc[rows_of(b), :].astype(BF16)
        return carry

    lax.fori_loop(0, num_layers, layer, 0)
    put = pltpu.make_async_copy(xs, out, io_sem)
    put.start()
    wait_sent(chunks - 2)
    wait_sent(chunks - 1)
    put.wait()


def solution(mesh):
    row_spec = P(("dp", "fsdp"), None, None)
    in_specs = (row_spec, P(("dp", "fsdp")), P(None, None, "fsdp"), P(None, "fsdp", None, None), P(None, "fsdp"),
                P(None, "fsdp", None), P(None, "fsdp"), P(None, "fsdp", None), P(None, "fsdp"), P(None, "fsdp", None),
                P(None, "fsdp"))
    n = mesh.shape["fsdp"]
    assert n % 2 == 0 and mesh.shape["dp"] % 2 == 0

    def local_step(hidden, lens, ln_par, w_qkv, b_qkv, w_out, b_out, w_up, b_up, w_down, b_down):
        _, seq, d_model = hidden.shape
        num_layers, tile, heads, triple = w_qkv.shape
        rps = w_down.shape[1] // tile
        assert hidden.shape[0] == 1 and n == 8 and n * tile == d_model and triple == 3 * tile and heads == n
        assert n * rps // 2 + 2 * (d_model // tile) == n * rps
        rot_half = tile // 8
        wide = 128
        raw_rows = 32 * heads
        dims = (n, num_layers, heads, tile, seq, d_model, rps, rot_half)
        chunks = num_layers * (heads + n * rps // 2 + d_model // tile)
        ring = n // 2
        vmem = pl.BlockSpec(memory_space=pltpu.VMEM)
        anywhere = pl.BlockSpec(memory_space=pl.ANY)
        dma = pltpu.SemaphoreType.DMA
        smalls = (ln_par, b_qkv, b_out, b_up, b_down)
        out, _, _ = pl.pallas_call(
            functools.partial(kernel, dims),
            name="layers",
            out_shape=(jax.ShapeDtypeStruct((seq, d_model), BF16),
                       jax.ShapeDtypeStruct((chunks, 3, n, tile, tile), BF16),
                       jax.ShapeDtypeStruct((num_layers, heads, tile, triple), BF16)),
            in_specs=[anywhere, pl.BlockSpec(memory_space=pltpu.SMEM), vmem] + [vmem] * 5 + [anywhere] * 4,
            out_specs=(anywhere, anywhere, anywhere),
            scratch_shapes=[
                pltpu.VMEM((seq, d_model), BF16),
                pltpu.VMEM((seq, d_model), BF16),
                pltpu.VMEM((seq, d_model), BF16),
                pltpu.VMEM((seq, d_model), BF16),
                pltpu.VMEM((rps, seq, d_model), BF16),
                pltpu.VMEM((seq, d_model), F32),
                pltpu.VMEM((seq, tile), BF16),
                pltpu.VMEM((seq, tile), BF16),
                pltpu.VMEM((seq, tile), BF16),
                pltpu.VMEM((2, 4, d_model, tile), BF16),
                pltpu.VMEM((3, seq, wide), F32),
                *[pltpu.VMEM((n,) + p.shape, p.dtype) for p in smalls],
                pltpu.VMEM((n, num_layers, 16, tile), F32),
                pltpu.VMEM((2, raw_rows, triple), BF16),
                pltpu.VMEM((raw_rows * triple // wide, wide), F32),
                pltpu.VMEM((2, heads, raw_rows // heads, triple), BF16),
                dma((SLOTS,)),
                dma((SLOTS, 3)),
                dma((SLOTS, 3)),
                dma((SLOTS, 3)),
                dma((SLOTS,)),
                dma((2, 4)),
                dma((5,)),
                dma((5,)),
                dma((2,)),
                dma((2,)),
                dma,
            ],
            compiler_params=pltpu.CompilerParams(
                collective_id=0, has_side_effects=True, vmem_limit_bytes=67043328),
        )(hidden.reshape(seq, d_model), lens, jnp.asarray(rope_row(2 * rot_half, wide)), *smalls,
          w_qkv.reshape(num_layers, tile * heads, triple), w_out, w_up, w_down)
        return out.reshape(1, seq, d_model)

    return jax.shard_map(local_step, mesh=mesh, in_specs=in_specs, out_specs=row_spec, check_vma=False)
```

```python
import functools

import jax
import jax.numpy as jnp
import numpy as np
from jax import lax
from jax.experimental import pallas as pl
from jax.experimental.pallas import tpu as pltpu
from jax.sharding import PartitionSpec as P

ROPE_BASE = 10000.0
LN_EPS = 1e-5
MESH = pl.DeviceIdType.MESH
SLOTS = 16
LATE = 4
ROWS = 256
DOT_ROWS = 256
F32 = jnp.float32
BF16 = jnp.bfloat16


def rope_row(rot_dim, width):
    inv_freq = np.float32(1.0) / (np.float32(ROPE_BASE) ** (np.arange(0, rot_dim, 2, dtype=np.float32) / np.float32(rot_dim)))
    lane = lax.broadcasted_iota(jnp.int32, (1, width), 1)
    row = jnp.zeros((1, width), F32)
    for i, value in enumerate(inv_freq):
        row = jnp.where((lane == i) | (lane == i + rot_dim // 2), float(value), row)
    return row


def kernel(dims, hid, lens, ln_own, bq_own, bo_own, bu_own, bd_own, wq_raw, wo, wu, wd, xs, gath, wq, a_s, m_s, ctx,
           act, acc, q_s, k_s, v_s, wbuf, tabs, ln_g, bq_g, bo_g, bu_g, bd_g, bias, raw, raw32, turned, send, rs, ls, ysem, dd,
           ld, small_send, small_recv, raw_in, raw_out, io_sem):
    n, num_layers, heads, tile, seq, d_model, rps, rot_half = dims
    ring = n // 2
    n_a, n_b, n_c = heads, n * rps // 2, d_model // tile
    per_layer = n_a + n_b + n_c
    chunks = num_layers * per_layer
    wide = tabs.shape[2]
    scale = float(tile) ** -0.5

    d, f = lax.axis_index("dp"), lax.axis_index("fsdp")
    x, c = f // 2, f % 2
    par = d % 2
    right = ((x + 1) % ring) * 2 + c
    left = ((x + ring - 1) % ring) * 2 + c
    far = ((x + 2) % ring) * 2 + c
    sib = x * 2 + 1 - c
    mate = d + 1 - 2 * par
    mine, other = 2 * par, 2 - 2 * par

    def remote(src, dst, s_sem, r_sem, where):
        return pltpu.make_async_remote_copy(
            src_ref=src, dst_ref=dst, send_sem=s_sem, recv_sem=r_sem, device_id=where, device_id_type=MESH)

    to_right, to_left, to_sib, to_mate = {"fsdp": right}, {"fsdp": left}, {"fsdp": sib}, {"dp": mate}

    def q_tile(l, h, i):
        return wq.at[l, h, :, pl.ds(i * tile, tile) if isinstance(i, int) else pl.ds(pl.multiple_of(i * tile, tile), tile)]

    def up_tile(l, u):
        return wu.at[l, :, pl.ds(pl.multiple_of((u % n) * (rps * tile) + (u // n) * tile, tile), tile)]

    def down_tile(l, v):
        return wd.at[l, pl.ds(pl.multiple_of((v // n_c) * tile, tile), tile),
                     pl.ds(pl.multiple_of((v % n_c) * tile, tile), tile)]

    def out_tile(l, j):
        return wo.at[l, :, pl.ds(pl.multiple_of(j * tile, tile), tile)]

    def with_own(k, go):
        l, r = k // per_layer, k % per_layer

        @pl.when(r < n_b)
        def _():
            go(lambda i: down_tile(l, r) if isinstance(i, int) and i == 1 else up_tile(l, 2 * r + i // 2))

        @pl.when((r >= n_b) & (r < n_b + n_a))
        def _():
            go(lambda i: q_tile(l, r - n_b, i))

        @pl.when(r >= n_a + n_b)
        def _():
            j = r - n_a - n_b
            go(lambda i: out_tile(l, j) if isinstance(i, int) and i == 1 else down_tile(l, n_b + 2 * j + i // 2))

    def own_first(k):
        slot = k % SLOTS

        def go(own):
            remote(own(mine), gath.at[k, mine, f], send.at[slot], rs.at[slot, 0], to_right).start()
            remote(own(1), gath.at[k, 1, f], send.at[slot], ls.at[slot, 0], to_left).start()
            for i in (mine, 1):
                remote(own(i), gath.at[k, i, f], send.at[slot], dd.at[slot], to_sib).start()

        with_own(k, go)

    def own_second(k):
        slot = k % SLOTS

        def go(own):
            remote(own(1), gath.at[k, 1, f], send.at[slot], rs.at[slot, 1], to_right).start()
            remote(own(mine), gath.at[k, mine, f], send.at[slot], ls.at[slot, 1], to_left).start()
            remote(own(other), gath.at[k, other, f], send.at[slot], dd.at[slot], to_sib).start()

        with_own(k, go)

    def wait_tile(sem):
        ref = gath.at[0, 0, 0]
        pltpu.make_async_copy(ref, ref, sem).wait()

    def pass_on(k, i, s, sem, where):
        t = gath.at[k, i, s]
        remote(t, t, send.at[k % SLOTS], sem, where).start()

    def from_sides(k):
        slot = k % SLOTS
        wait_tile(rs.at[slot, 0])
        pass_on(k, mine, left, rs.at[slot, 2], to_right)
        pass_on(k, mine, left, ysem.at[slot, 0], to_mate)
        pass_on(k, mine, left, dd.at[slot], to_sib)
        wait_tile(ls.at[slot, 0])
        pass_on(k, 1, right, ls.at[slot, 2], to_left)
        pass_on(k, 1, right, dd.at[slot], to_sib)

    def from_sides_again(k):
        slot = k % SLOTS
        wait_tile(ls.at[slot, 1])
        pass_on(k, mine, right, ysem.at[slot, 1], to_mate)
        pass_on(k, mine, right, dd.at[slot], to_sib)
        wait_tile(rs.at[slot, 1])
        pass_on(k, 1, left, dd.at[slot], to_sib)

    def from_far(k):
        slot = k % SLOTS
        wait_tile(rs.at[slot, 2])
        pass_on(k, mine, far, ysem.at[slot, 2], to_mate)
        pass_on(k, mine, far, dd.at[slot], to_sib)
        wait_tile(ls.at[slot, 2])
        pass_on(k, 1, far, dd.at[slot], to_sib)

    def from_mate(i, s):
        def do(k):
            slot = k % SLOTS
            wait_tile(ysem.at[slot, i])
            pass_on(k, other, s, dd.at[slot], to_sib)

        return do

    sib_tiles = 3 * ring
    sent_tiles = 3 * (ring - 1) + sib_tiles

    def wait_sib(k):
        ref = gath.at[0, :, pl.ds(0, sib_tiles // 3)]
        pltpu.make_async_copy(ref, ref, dd.at[k % SLOTS]).wait()

    def wait_sent(k):
        ref = gath.at[0, :, pl.ds(0, sent_tiles // 3)]
        pltpu.make_async_copy(ref, ref, send.at[k % SLOTS]).wait()

    def load_tile(k, kk, i, to, own):
        slot = k % 2
        for step in range(1, n):
            s = (f + step) % n
            pltpu.make_async_copy(
                gath.at[kk, i, s], wbuf.at[slot, to, pl.ds(pl.multiple_of(s * tile, tile), tile)], ld.at[slot, to]).start()
        pltpu.make_async_copy(own, wbuf.at[slot, to, pl.ds(pl.multiple_of(f * tile, tile), tile)], ld.at[slot, to]).start()

    def load(k):
        l, r = k // per_layer, k % per_layer
        j = r - n_a - n_b

        @pl.when(r < n_b)
        def _():
            for i in (0, 2):
                load_tile(k, k, i, i, up_tile(l, 2 * r + i // 2))

        @pl.when((r >= LATE) & (r < n_b))
        def _():
            load_tile(k, k - LATE, 1, 3, down_tile(l, r - LATE))

        @pl.when((r >= n_b) & (r < n_b + n_a))
        def _():
            for i in range(3):
                load_tile(k, k, i, i, q_tile(l, r - n_b, i))

        @pl.when(r >= n_a + n_b)
        def _():
            load_tile(k, k, 0, 0, down_tile(l, n_b + 2 * j))
            load_tile(k, k, 1, 1, out_tile(l, j))
            load_tile(k, k, 2, 2, down_tile(l, n_b + 2 * j + 1))

        @pl.when((r >= n_a + n_b) & (j < LATE))
        def _():
            load_tile(k, k - n_a - LATE, 1, 3, down_tile(l, n_b - LATE + j))

    def loaded(slot, to):
        pltpu.make_async_copy(wbuf.at[slot, to], wbuf.at[slot, to], ld.at[slot, to]).wait()

    def within(k, do):
        @pl.when((k >= 0) & (k < chunks))
        def _():
            do(k)

    def part0(t):
        within(t - 7, wait_sent)
        within(t, own_first)
        within(t - 2, from_sides_again)

    def part1(t):
        within(t - 1, from_sides)
        within(t - 2, from_far)
        within(t - 3, from_mate(1, right))
        within(t - 3, from_mate(2, far))

    def part2(t):
        within(t, own_second)
        within(t - 2, from_mate(0, left))
        within(t - 3, wait_sib)
        within(t - 3, load)

    blocks = seq // ROWS

    def rows_of(b):
        return pl.ds(b * ROWS, ROWS)

    dot_blocks = [pl.ds(b * DOT_ROWS, DOT_ROWS) for b in range(seq // DOT_ROWS)]

    def cols_of(j):
        return pl.ds(pl.multiple_of(j * tile, tile), tile)

    def row(s, l, i):
        return bias[s, l, pl.ds(i, 1), :]

    def ln_row(s, l, i):
        return ln_g[s, l, pl.ds(i, 1), :]

    norm_rows = 128

    def layer_norms(l, first, last):
        step = norm_rows

        def body(b, carry):
            rows = pl.ds(pl.multiple_of(b * step, step), step)
            v = xs[rows, :].astype(F32)
            cen = v - jnp.mean(v, axis=-1, keepdims=True)
            inv = lax.rsqrt(jnp.mean(cen * cen, axis=-1, keepdims=True) + LN_EPS)
            for s in range(n):
                cols = pl.ds(s * tile, tile)
                norm = cen[:, s * tile:(s + 1) * tile] * inv
                a_s[rows, cols] = (norm * ln_row(s, l, 0) + ln_row(s, l, 1)).astype(BF16)
                m_s[rows, cols] = (norm * ln_row(s, l, 2) + ln_row(s, l, 3)).astype(BF16)
                acc[rows, cols] = v[:, s * tile:(s + 1) * tile] + (row(s, l, 3) + row(s, l, 4 + rps))
            return carry

        lax.fori_loop(first, last, body, 0)

    def dot(lhs, slot, to):
        return jnp.dot(lhs, wbuf[slot, to], preferred_element_type=F32)

    def rotate(v, rows):
        u = v[:, :wide].astype(F32)
        turned = (u * tabs[0, rows, :] + pltpu.roll(u, wide - rot_half, 1) * tabs[1, rows, :]
                  + pltpu.roll(u, rot_half, 1) * tabs[2, rows, :])
        return turned.astype(BF16)

    def project(l, h, slot, i, ref):
        for rows in dot_blocks:
            v = (dot(a_s[rows, :], slot, i) + row(h, l, i)).astype(BF16)
            if i < 2:
                ref[rows, pl.ds(0, wide)] = rotate(v, rows)
                ref[rows, pl.ds(wide, tile - wide)] = v[:, wide:]
            else:
                ref[rows, :] = v

    def attend(h, b):
        width = (b + 1) * ROWS
        s = lax.dot_general(q_s[rows_of(b), :], k_s[pl.ds(0, width), :], (((1,), (1,)), ((), ())),
                            preferred_element_type=F32) * scale
        col = lax.broadcasted_iota(jnp.int32, (ROWS, width), 1)
        at = lax.broadcasted_iota(jnp.int32, (ROWS, width), 0) + b * ROWS
        s = jnp.where((col <= at) & (col < lens[0]), s, -1e30)
        e = jnp.exp(s - jnp.max(s, axis=-1, keepdims=True))
        p = (e * (1.0 / jnp.sum(e, axis=-1, keepdims=True))).astype(BF16)
        ctx[rows_of(b), cols_of(h)] = jnp.dot(p, v_s[pl.ds(0, width), :], preferred_element_type=F32).astype(BF16)

    def up(l, u, slot, to):
        s, rp = u % n, u // n
        for rows in dot_blocks:
            v = dot(m_s[rows, :], slot, to) + row(s, l, 4 + rp)
            g = (0.5 * v) * (1.0 + lax.erf(v * (0.5 ** 0.5)))
            act[rp, rows, cols_of(s)] = g.astype(BF16)

    def add_to(j, slot, to, lhs):
        for rows in dot_blocks:
            acc[rows, cols_of(j)] += dot(lhs(rows), slot, to)

    def down(v, slot, to):
        add_to(v % n_c, slot, to, lambda rows: act[v // n_c, rows, :])

    def head_step(l, h):
        k = l * per_layer + n_b + h
        slot = k % 2
        part0(k + 4)
        loaded(slot, 0)
        loaded(slot, 1)
        project(l, h, slot, 0, q_s)
        project(l, h, slot, 1, k_s)
        part1(k + 4)
        loaded(slot, 2)
        project(l, h, slot, 2, v_s)
        for b in range(blocks // 2):
            attend(h, b)
        part2(k + 4)
        for b in range(blocks // 2, blocks):
            attend(h, b)

    def up_step(l, j):
        k = l * per_layer + j
        slot = k % 2
        part0(k + 4)
        loaded(slot, 0)
        up(l, 2 * j, slot, 0)
        part1(k + 4)
        loaded(slot, 2)
        up(l, 2 * j + 1, slot, 2)
        part2(k + 4)

        @pl.when(j >= LATE)
        def _():
            loaded(slot, 3)
            down(j - LATE, slot, 3)

    def down_step(l, j):
        k = l * per_layer + n_a + n_b + j
        slot = k % 2
        part0(k + 4)
        loaded(slot, 0)
        down(n_b + 2 * j, slot, 0)

        @pl.when(j < LATE)
        def _():
            loaded(slot, 3)
            down(n_b - LATE + j, slot, 3)

        part1(k + 4)
        loaded(slot, 2)
        down(n_b + 2 * j + 1, slot, 2)
        part2(k + 4)
        loaded(slot, 1)
        add_to(j, slot, 1, lambda rows: ctx[rows, :])

    def rotary_tables():
        freq = rope_row(2 * rot_half, wide)
        for b in range(blocks):
            at = (lax.broadcasted_iota(jnp.int32, (ROWS, wide), 0) + b * ROWS).astype(F32)
            lane = lax.broadcasted_iota(jnp.int32, (ROWS, wide), 1)
            angle = at * freq
            cos, sin = jnp.cos(angle), jnp.sin(angle)
            tabs[0, rows_of(b), :] = jnp.where(lane < 2 * rot_half, cos, 1.0)
            tabs[1, rows_of(b), :] = jnp.where(lane < rot_half, -sin, 0.0)
            tabs[2, rows_of(b), :] = jnp.where((lane >= rot_half) & (lane < 2 * rot_half), sin, 0.0)

    raw_rows = raw.shape[1]
    per_raw = tile * heads // raw_rows
    raws = num_layers * per_raw

    def get_raw(b):
        return pltpu.make_async_copy(
            wq_raw.at[b // per_raw, pl.ds(pl.multiple_of((b % per_raw) * raw_rows, raw_rows), raw_rows)],
            raw.at[b % 2], raw_in.at[b % 2])

    def put_raw(b):
        some = raw_rows // heads
        return pltpu.make_async_copy(
            turned.at[b % 2], wq.at[b // per_raw, :, pl.ds(pl.multiple_of((b % per_raw) * some, some), some)],
            raw_out.at[b % 2])

    def by_head(first, last):
        def body(b, carry):
            get_raw(b).wait()
            for q in range(raw.shape[2] // wide):
                raw32[pl.ds(q * raw_rows, raw_rows), :] = raw[b % 2, :, pl.ds(q * wide, wide)].astype(F32)

            @pl.when(b + 2 < raws)
            def _():
                get_raw(b + 2).start()

            @pl.when(b >= 2)
            def _():
                put_raw(b - 2).wait()

            for h in range(heads):
                for q in range(raw.shape[2] // wide):
                    turned[b % 2, h, :, pl.ds(q * wide, wide)] = (
                        raw32[pl.ds(q * raw_rows + h, raw_rows // heads, stride=heads), :].astype(BF16))
            put_raw(b).start()
            return carry

        lax.fori_loop(first, last, body, 0)

    def unpack_biases():
        for s in range(n):
            for g, at, count in ((bq_g, 0, 3), (bo_g, 3, 1), (bu_g, 4, rps), (bd_g, 4 + rps, 1)):
                for i in range(count):
                    v = g[s, :, pl.ds(i * tile, tile)].astype(F32)
                    for l in range(num_layers):
                        bias[s, l, pl.ds(at + i, 1), :] = v[l:l + 1]

    get_hidden = pltpu.make_async_copy(hid, xs, io_sem)
    get_hidden.start()
    get_raw(0).start()
    get_raw(1).start()
    barrier = pltpu.get_barrier_semaphore()
    for step in range(1, n):
        pl.semaphore_signal(barrier, inc=1, device_id={"fsdp": (f + step) % n}, device_id_type=MESH)
    pl.semaphore_signal(barrier, inc=1, device_id=to_mate, device_id_type=MESH)
    pl.semaphore_wait(barrier, n)

    smalls = ((ln_own, ln_g), (bq_own, bq_g), (bo_own, bo_g), (bu_own, bu_g), (bd_own, bd_g))
    for i, (own, everyone) in enumerate(smalls):
        for step in range(1, n):
            remote(own, everyone.at[f], small_send.at[i], small_recv.at[i], {"fsdp": (f + step) % n}).start()
    own_first(0)
    own_second(0)
    part0(1)
    for own, everyone in smalls:
        everyone[f] = own[...]
    rotary_tables()
    part1(1)
    for i, (own, everyone) in enumerate(smalls):
        ref = everyone.at[pl.ds(0, n - 1)]
        pltpu.make_async_copy(ref, ref, small_send.at[i]).wait()
        pltpu.make_async_copy(ref, ref, small_recv.at[i]).wait()
    unpack_biases()
    part2(1)
    get_hidden.wait()
    norms = seq // norm_rows
    for i, part in enumerate((part0, part1, part2, part0)):
        layer_norms(0, norms * i // 4, norms * (i + 1) // 4)
        part(2 + i // 3)
    by_head(0, raws // 3)
    part1(3)
    by_head(raws // 3, raws * 2 // 3)
    part2(3)
    by_head(raws * 2 // 3, raws)
    put_raw(raws - 2).wait()
    put_raw(raws - 1).wait()

    def layer(l, carry):
        def loop(count, step):
            def body(i, inner):
                step(l, i)
                return inner

            lax.fori_loop(0, count, body, 0)

        @pl.when(l > 0)
        def _():
            layer_norms(l, 0, seq // norm_rows)

        loop(n_b, up_step)
        loop(n_a, head_step)
        loop(n_c, down_step)
        for b in range(blocks):
            xs[rows_of(b), :] = acc[rows_of(b), :].astype(BF16)
        return carry

    lax.fori_loop(0, num_layers, layer, 0)
    for k in range(chunks - 3, chunks):
        wait_sent(k)


def solution(mesh):
    row_spec = P(("dp", "fsdp"), None, None)
    in_specs = (row_spec, P(("dp", "fsdp")), P(None, None, "fsdp"), P(None, "fsdp", None, None), P(None, "fsdp"),
                P(None, "fsdp", None), P(None, "fsdp"), P(None, "fsdp", None), P(None, "fsdp"), P(None, "fsdp", None),
                P(None, "fsdp"))
    n = mesh.shape["fsdp"]
    assert n % 2 == 0 and mesh.shape["dp"] % 2 == 0

    def local_step(hidden, lens, ln_par, w_qkv, b_qkv, w_out, b_out, w_up, b_up, w_down, b_down):
        _, seq, d_model = hidden.shape
        num_layers, tile, heads, triple = w_qkv.shape
        rps = w_down.shape[1] // tile
        assert hidden.shape[0] == 1 and n == 8 and n * tile == d_model and triple == 3 * tile and heads == n
        assert n * rps // 2 + 2 * (d_model // tile) == n * rps
        rot_half = tile // 8
        wide = 128
        raw_rows = 32 * heads
        dims = (n, num_layers, heads, tile, seq, d_model, rps, rot_half)
        chunks = num_layers * (heads + n * rps // 2 + d_model // tile)
        ring = n // 2
        vmem = pl.BlockSpec(memory_space=pltpu.VMEM)
        anywhere = pl.BlockSpec(memory_space=pl.ANY)
        dma = pltpu.SemaphoreType.DMA
        smalls = (ln_par, b_qkv, b_out, b_up, b_down)
        out, _, _ = pl.pallas_call(
            functools.partial(kernel, dims),
            name="layers",
            out_shape=(pltpu.VMEM((seq, d_model), BF16),
                       jax.ShapeDtypeStruct((chunks, 3, n, tile, tile), BF16),
                       jax.ShapeDtypeStruct((num_layers, heads, tile, triple), BF16)),
            in_specs=[anywhere, pl.BlockSpec(memory_space=pltpu.SMEM)] + [vmem] * 5 + [anywhere] * 4,
            out_specs=(vmem, anywhere, anywhere),
            scratch_shapes=[
                pltpu.VMEM((seq, d_model), BF16),
                pltpu.VMEM((seq, d_model), BF16),
                pltpu.VMEM((seq, d_model), BF16),
                pltpu.VMEM((rps, seq, d_model), BF16),
                pltpu.VMEM((seq, d_model), F32),
                pltpu.VMEM((seq, tile), BF16),
                pltpu.VMEM((seq, tile), BF16),
                pltpu.VMEM((seq, tile), BF16),
                pltpu.VMEM((2, 4, d_model, tile), BF16),
                pltpu.VMEM((3, seq, wide), F32),
                *[pltpu.VMEM((n,) + p.shape, p.dtype) for p in smalls],
                pltpu.VMEM((n, num_layers, 16, tile), F32),
                pltpu.VMEM((2, raw_rows, triple), BF16),
                pltpu.VMEM((raw_rows * triple // wide, wide), F32),
                pltpu.VMEM((2, heads, raw_rows // heads, triple), BF16),
                dma((SLOTS,)),
                dma((SLOTS, 3)),
                dma((SLOTS, 3)),
                dma((SLOTS, 3)),
                dma((SLOTS,)),
                dma((2, 4)),
                dma((5,)),
                dma((5,)),
                dma((2,)),
                dma((2,)),
                dma,
            ],
            compiler_params=pltpu.CompilerParams(
                collective_id=0, has_side_effects=True, vmem_limit_bytes=59 * 2**20),
        )(hidden.reshape(seq, d_model), lens, *smalls,
          w_qkv.reshape(num_layers, tile * heads, triple), w_out, w_up, w_down)
        return out.reshape(1, seq, d_model)

    return jax.shard_map(local_step, mesh=mesh, in_specs=in_specs, out_specs=row_spec, check_vma=False)
```

```python
import functools

import jax
import jax.numpy as jnp
import numpy as np
from jax import lax
from jax.experimental import pallas as pl
from jax.experimental.pallas import tpu as pltpu
from jax.sharding import PartitionSpec as P

ROPE_BASE = 10000.0
LN_EPS = 1e-5
MESH = pl.DeviceIdType.MESH
SLOTS = 16
AHEAD = 1
LATE = 4
ROWS = 256
DOT_ROWS = 256
F32 = jnp.float32
BF16 = jnp.bfloat16


def rope_row(rot_dim, width):
    inv_freq = np.float32(1.0) / (np.float32(ROPE_BASE) ** (np.arange(0, rot_dim, 2, dtype=np.float32) / np.float32(rot_dim)))
    lane = lax.broadcasted_iota(jnp.int32, (1, width), 1)
    row = jnp.zeros((1, width), F32)
    for i, value in enumerate(inv_freq):
        row = jnp.where((lane == i) | (lane == i + rot_dim // 2), float(value), row)
    return row


def kernel(dims, hid, lens, ln_own, bq_own, bo_own, bu_own, bd_own, wq_raw, wo, wu, wd, xs, gath, wq, a_s, m_s, ctx,
           act, acc, q_s, k_s, v_s, wbuf, tabs, ln_g, bq_g, bo_g, bu_g, bd_g, bias, raw, raw32, turned, send, rs, ls, ysem, dd,
           ld, small_send, small_recv, raw_in, raw_out, io_sem):
    n, num_layers, heads, tile, seq, d_model, rps, rot_half = dims
    ring = n // 2
    n_a, n_b, n_c = heads, n * rps // 2, d_model // tile
    per_layer = n_a + n_b + n_c
    chunks = num_layers * per_layer
    wide = tabs.shape[2]
    scale = float(tile) ** -0.5

    d, f = lax.axis_index("dp"), lax.axis_index("fsdp")
    x, c = f // 2, f % 2
    par = d % 2
    right = ((x + 1) % ring) * 2 + c
    left = ((x + ring - 1) % ring) * 2 + c
    far = ((x + 2) % ring) * 2 + c
    sib = x * 2 + 1 - c
    mate = d + 1 - 2 * par
    mine, other = 2 * par, 2 - 2 * par

    def remote(src, dst, s_sem, r_sem, where):
        return pltpu.make_async_remote_copy(
            src_ref=src, dst_ref=dst, send_sem=s_sem, recv_sem=r_sem, device_id=where, device_id_type=MESH)

    to_right, to_left, to_sib, to_mate = {"fsdp": right}, {"fsdp": left}, {"fsdp": sib}, {"dp": mate}

    def q_tile(l, h, i):
        return wq.at[l, h, :, pl.ds(i * tile, tile) if isinstance(i, int) else pl.ds(pl.multiple_of(i * tile, tile), tile)]

    def up_tile(l, u):
        return wu.at[l, :, pl.ds(pl.multiple_of((u % n) * (rps * tile) + (u // n) * tile, tile), tile)]

    def down_tile(l, v):
        return wd.at[l, pl.ds(pl.multiple_of((v // n_c) * tile, tile), tile),
                     pl.ds(pl.multiple_of((v % n_c) * tile, tile), tile)]

    def out_tile(l, j):
        return wo.at[l, :, pl.ds(pl.multiple_of(j * tile, tile), tile)]

    def with_own(k, go):
        l, r = k // per_layer, k % per_layer

        @pl.when(r < n_b)
        def _():
            go(lambda i: down_tile(l, r) if isinstance(i, int) and i == 1 else up_tile(l, 2 * r + i // 2))

        @pl.when((r >= n_b) & (r < n_b + n_a))
        def _():
            go(lambda i: q_tile(l, r - n_b, i))

        @pl.when(r >= n_a + n_b)
        def _():
            j = r - n_a - n_b
            go(lambda i: out_tile(l, j) if isinstance(i, int) and i == 1 else down_tile(l, n_b + 2 * j + i // 2))

    def own_first(k):
        slot = k % SLOTS

        def go(own):
            remote(own(mine), gath.at[k, mine, f], send.at[slot], rs.at[slot, 0], to_right).start()
            remote(own(1), gath.at[k, 1, f], send.at[slot], ls.at[slot, 0], to_left).start()
            for role, i in enumerate((mine, 1)):
                remote(own(i), gath.at[k, i, f], send.at[slot], dd.at[slot, role], to_sib).start()

        with_own(k, go)

    def own_second(k):
        slot = k % SLOTS

        def go(own):
            remote(own(1), gath.at[k, 1, f], send.at[slot], rs.at[slot, 1], to_right).start()
            remote(own(mine), gath.at[k, mine, f], send.at[slot], ls.at[slot, 1], to_left).start()
            remote(own(other), gath.at[k, other, f], send.at[slot], dd.at[slot, 2], to_sib).start()

        with_own(k, go)

    def wait_tile(sem):
        ref = gath.at[0, 0, 0]
        pltpu.make_async_copy(ref, ref, sem).wait()

    def pass_on(k, i, s, sem, where):
        t = gath.at[k, i, s]
        remote(t, t, send.at[k % SLOTS], sem, where).start()

    def from_sides(k):
        slot = k % SLOTS
        wait_tile(rs.at[slot, 0])
        pass_on(k, mine, left, rs.at[slot, 2], to_right)
        pass_on(k, mine, left, ysem.at[slot, 0], to_mate)
        pass_on(k, mine, left, dd.at[slot, 0], to_sib)
        wait_tile(ls.at[slot, 0])
        pass_on(k, 1, right, ls.at[slot, 2], to_left)
        pass_on(k, 1, right, dd.at[slot, 1], to_sib)

    def from_sides_again(k):
        slot = k % SLOTS
        wait_tile(ls.at[slot, 1])
        pass_on(k, mine, right, ysem.at[slot, 1], to_mate)
        pass_on(k, mine, right, dd.at[slot, 0], to_sib)
        wait_tile(rs.at[slot, 1])
        pass_on(k, 1, left, dd.at[slot, 1], to_sib)

    def from_far(k):
        slot = k % SLOTS
        wait_tile(rs.at[slot, 2])
        pass_on(k, mine, far, ysem.at[slot, 2], to_mate)
        pass_on(k, mine, far, dd.at[slot, 0], to_sib)
        wait_tile(ls.at[slot, 2])
        pass_on(k, 1, far, dd.at[slot, 1], to_sib)

    def from_mate(i, s):
        def do(k):
            slot = k % SLOTS
            wait_tile(ysem.at[slot, i])
            pass_on(k, other, s, dd.at[slot, 2], to_sib)

        return do

    sent_tiles = 3 * (ring - 1) + 3 * ring

    def wait_sib(k, role):
        ref = gath.at[0, 0, pl.ds(0, ring)]
        pltpu.make_async_copy(ref, ref, dd.at[k % SLOTS, role]).wait()

    def wait_sent(k):
        ref = gath.at[0, :, pl.ds(0, sent_tiles // 3)]
        pltpu.make_async_copy(ref, ref, send.at[k % SLOTS]).wait()

    def load_tile(k, kk, i, to, own):
        slot = k % 2
        for step in range(1, n):
            s = (f + step) % n
            pltpu.make_async_copy(
                gath.at[kk, i, s], wbuf.at[slot, to, pl.ds(pl.multiple_of(s * tile, tile), tile)], ld.at[slot, to]).start()
        pltpu.make_async_copy(own, wbuf.at[slot, to, pl.ds(pl.multiple_of(f * tile, tile), tile)], ld.at[slot, to]).start()

    def load_down(k, i):
        j = k % per_layer - n_a - n_b
        load_tile(k, k, i, i, down_tile(k // per_layer, n_b + 2 * j + i // 2))

    def load(k):
        wait_sib(k, 0)
        wait_sib(k, 1)

        @pl.when(k < chunks - 1)
        def _():
            wait_sib(k, 2)

        l, r = k // per_layer, k % per_layer
        j = r - n_a - n_b

        @pl.when(r < n_b)
        def _():
            for i in (0, 2):
                load_tile(k, k, i, i, up_tile(l, 2 * r + i // 2))

        @pl.when((r >= LATE) & (r < n_b))
        def _():
            load_tile(k, k - LATE, 1, 3, down_tile(l, r - LATE))

        @pl.when((r >= n_b) & (r < n_b + n_a))
        def _():
            for i in range(3):
                load_tile(k, k, i, i, q_tile(l, r - n_b, i))

        @pl.when(r >= n_a + n_b)
        def _():
            load_tile(k, k, 1, 1, out_tile(l, j))
            load_down(k, mine)

        @pl.when((r >= n_a + n_b) & (k < chunks - 1))
        def _():
            load_down(k, other)

        @pl.when((r >= n_a + n_b) & (j < LATE))
        def _():
            load_tile(k, k - n_a - LATE, 1, 3, down_tile(l, n_b - LATE + j))

    def loaded(slot, to):
        pltpu.make_async_copy(wbuf.at[slot, to], wbuf.at[slot, to], ld.at[slot, to]).wait()

    def within(k, do, end=chunks):
        @pl.when((k >= 0) & (k < end))
        def _():
            do(k)

    def part0(t):
        within(t - 7, wait_sent)
        within(t + AHEAD, own_first)
        within(t - 2, from_sides_again)

    def part1(t):
        within(t - 1, from_sides)
        within(t - 2, from_far)
        within(t - 3, from_mate(1, right))
        within(t - 3, from_mate(2, far), chunks - 1)

    def part2(t):
        within(t + AHEAD, own_second)
        within(t - 2, from_mate(0, left))
        within(t - 3, load)

    blocks = seq // ROWS

    def rows_of(b):
        return pl.ds(b * ROWS, ROWS)

    dot_blocks = [pl.ds(b * DOT_ROWS, DOT_ROWS) for b in range(seq // DOT_ROWS)]

    def cols_of(j):
        return pl.ds(pl.multiple_of(j * tile, tile), tile)

    def row(s, l, i):
        return bias[s, l, pl.ds(i, 1), :]

    def ln_row(s, l, i):
        return ln_g[s, l, pl.ds(i, 1), :]

    norm_rows = 128

    def layer_norms(l, first, last):
        step = norm_rows

        def body(b, carry):
            rows = pl.ds(pl.multiple_of(b * step, step), step)
            v = xs[rows, :].astype(F32)
            cen = v - jnp.mean(v, axis=-1, keepdims=True)
            inv = lax.rsqrt(jnp.mean(cen * cen, axis=-1, keepdims=True) + LN_EPS)
            for s in range(n):
                cols = pl.ds(s * tile, tile)
                norm = cen[:, s * tile:(s + 1) * tile] * inv
                a_s[rows, cols] = (norm * ln_row(s, l, 0) + ln_row(s, l, 1)).astype(BF16)
                m_s[rows, cols] = (norm * ln_row(s, l, 2) + ln_row(s, l, 3)).astype(BF16)
                acc[rows, cols] = v[:, s * tile:(s + 1) * tile] + (row(s, l, 3) + row(s, l, 4 + rps))
            return carry

        lax.fori_loop(first, last, body, 0)

    def dot(lhs, slot, to):
        return jnp.dot(lhs, wbuf[slot, to], preferred_element_type=F32)

    def rotate(v, rows):
        u = v[:, :wide].astype(F32)
        turned = (u * tabs[0, rows, :] + pltpu.roll(u, wide - rot_half, 1) * tabs[1, rows, :]
                  + pltpu.roll(u, rot_half, 1) * tabs[2, rows, :])
        return turned.astype(BF16)

    def project(l, h, slot, i, ref):
        for rows in dot_blocks:
            v = (dot(a_s[rows, :], slot, i) + row(h, l, i)).astype(BF16)
            if i < 2:
                ref[rows, pl.ds(0, wide)] = rotate(v, rows)
                ref[rows, pl.ds(wide, tile - wide)] = v[:, wide:]
            else:
                ref[rows, :] = v

    def attend(h, b):
        width = (b + 1) * ROWS
        s = lax.dot_general(q_s[rows_of(b), :], k_s[pl.ds(0, width), :], (((1,), (1,)), ((), ())),
                            preferred_element_type=F32) * scale
        col = lax.broadcasted_iota(jnp.int32, (ROWS, width), 1)
        at = lax.broadcasted_iota(jnp.int32, (ROWS, width), 0) + b * ROWS
        s = jnp.where((col <= at) & (col < lens[0]), s, -1e30)
        e = jnp.exp(s - jnp.max(s, axis=-1, keepdims=True))
        p = (e * (1.0 / jnp.sum(e, axis=-1, keepdims=True))).astype(BF16)
        ctx[rows_of(b), cols_of(h)] = jnp.dot(p, v_s[pl.ds(0, width), :], preferred_element_type=F32).astype(BF16)

    def up(l, u, slot, to):
        s, rp = u % n, u // n
        for rows in dot_blocks:
            v = dot(m_s[rows, :], slot, to) + row(s, l, 4 + rp)
            g = (0.5 * v) * (1.0 + lax.erf(v * (0.5 ** 0.5)))
            act[rp, rows, cols_of(s)] = g.astype(BF16)

    def add_to(j, slot, to, lhs):
        for rows in dot_blocks:
            acc[rows, cols_of(j)] += dot(lhs(rows), slot, to)

    def down(v, slot, to):
        add_to(v % n_c, slot, to, lambda rows: act[v // n_c, rows, :])

    def head_step(l, h):
        k = l * per_layer + n_b + h
        slot = k % 2
        part0(k + 4)
        loaded(slot, 0)
        loaded(slot, 1)
        project(l, h, slot, 0, q_s)
        project(l, h, slot, 1, k_s)
        part1(k + 4)
        loaded(slot, 2)
        project(l, h, slot, 2, v_s)
        for b in range(blocks // 2):
            attend(h, b)
        part2(k + 4)
        for b in range(blocks // 2, blocks):
            attend(h, b)

    def up_step(l, j):
        k = l * per_layer + j
        slot = k % 2
        part0(k + 4)
        loaded(slot, 0)
        up(l, 2 * j, slot, 0)
        part1(k + 4)
        loaded(slot, 2)
        up(l, 2 * j + 1, slot, 2)
        part2(k + 4)

        @pl.when(j >= LATE)
        def _():
            loaded(slot, 3)
            down(j - LATE, slot, 3)

    def down_step(l, j):
        k = l * per_layer + n_a + n_b + j
        slot = k % 2
        part0(k + 4)
        loaded(slot, 1)
        add_to(j, slot, 1, lambda rows: ctx[rows, :])

        @pl.when(j < LATE)
        def _():
            loaded(slot, 3)
            down(n_b - LATE + j, slot, 3)

        part1(k + 4)
        loaded(slot, mine)
        down(n_b + 2 * j + mine // 2, slot, mine)
        part2(k + 4)

        @pl.when(k == chunks - 1)
        def _():
            from_mate(2, far)(k)
            wait_sib(k, 2)
            load_down(k, other)

        loaded(slot, other)
        down(n_b + 2 * j + other // 2, slot, other)

        @pl.when(j >= n_c // 2)
        def _():
            cols = pl.ds(pl.multiple_of((2 * j - n_c) * tile, 2 * tile), 2 * tile)
            for b in range(blocks):
                xs[rows_of(b), cols] = acc[rows_of(b), cols].astype(BF16)

    def rotary_tables():
        freq = rope_row(2 * rot_half, wide)
        for b in range(blocks):
            at = (lax.broadcasted_iota(jnp.int32, (ROWS, wide), 0) + b * ROWS).astype(F32)
            lane = lax.broadcasted_iota(jnp.int32, (ROWS, wide), 1)
            angle = at * freq
            cos, sin = jnp.cos(angle), jnp.sin(angle)
            tabs[0, rows_of(b), :] = jnp.where(lane < 2 * rot_half, cos, 1.0)
            tabs[1, rows_of(b), :] = jnp.where(lane < rot_half, -sin, 0.0)
            tabs[2, rows_of(b), :] = jnp.where((lane >= rot_half) & (lane < 2 * rot_half), sin, 0.0)

    raw_rows = raw.shape[1]
    per_raw = tile * heads // raw_rows
    raws = num_layers * per_raw

    def get_raw(b):
        return pltpu.make_async_copy(
            wq_raw.at[b // per_raw, pl.ds(pl.multiple_of((b % per_raw) * raw_rows, raw_rows), raw_rows)],
            raw.at[b % 2], raw_in.at[b % 2])

    def put_raw(b):
        some = raw_rows // heads
        return pltpu.make_async_copy(
            turned.at[b % 2], wq.at[b // per_raw, :, pl.ds(pl.multiple_of((b % per_raw) * some, some), some)],
            raw_out.at[b % 2])

    def by_head(first, last):
        def body(b, carry):
            get_raw(b).wait()
            for q in range(raw.shape[2] // wide):
                raw32[pl.ds(q * raw_rows, raw_rows), :] = raw[b % 2, :, pl.ds(q * wide, wide)].astype(F32)

            @pl.when(b + 2 < raws)
            def _():
                get_raw(b + 2).start()

            @pl.when(b >= 2)
            def _():
                put_raw(b - 2).wait()

            for h in range(heads):
                for q in range(raw.shape[2] // wide):
                    turned[b % 2, h, :, pl.ds(q * wide, wide)] = (
                        raw32[pl.ds(q * raw_rows + h, raw_rows // heads, stride=heads), :].astype(BF16))
            put_raw(b).start()
            return carry

        lax.fori_loop(first, last, body, 0)

    def unpack_biases():
        for s in range(n):
            for g, at, count in ((bq_g, 0, 3), (bo_g, 3, 1), (bu_g, 4, rps), (bd_g, 4 + rps, 1)):
                for i in range(count):
                    v = g[s, :, pl.ds(i * tile, tile)].astype(F32)
                    for l in range(num_layers):
                        bias[s, l, pl.ds(at + i, 1), :] = v[l:l + 1]

    get_hidden = pltpu.make_async_copy(hid, xs, io_sem)
    get_hidden.start()
    get_raw(0).start()
    get_raw(1).start()
    barrier = pltpu.get_barrier_semaphore()
    for step in range(1, n):
        pl.semaphore_signal(barrier, inc=1, device_id={"fsdp": (f + step) % n}, device_id_type=MESH)
    pl.semaphore_signal(barrier, inc=1, device_id=to_mate, device_id_type=MESH)
    pl.semaphore_wait(barrier, n)

    smalls = ((ln_own, ln_g), (bq_own, bq_g), (bo_own, bo_g), (bu_own, bu_g), (bd_own, bd_g))
    own_first(0)
    for i, (own, everyone) in enumerate(smalls):
        for step in range(1, n):
            remote(own, everyone.at[f], small_send.at[i], small_recv.at[i], {"fsdp": (f + step) % n}).start()
    own_second(0)
    part0(0)
    part2(0)
    part0(1)
    for own, everyone in smalls:
        everyone[f] = own[...]
    rotary_tables()
    part1(1)
    for i, (own, everyone) in enumerate(smalls):
        ref = everyone.at[pl.ds(0, n - 1)]
        pltpu.make_async_copy(ref, ref, small_send.at[i]).wait()
        pltpu.make_async_copy(ref, ref, small_recv.at[i]).wait()
    unpack_biases()
    part2(1)
    get_hidden.wait()
    norms = seq // norm_rows
    for i, part in enumerate((part0, part1, part2, part0)):
        layer_norms(0, norms * i // 4, norms * (i + 1) // 4)
        part(2 + i // 3)
    by_head(0, raws // 3)
    part1(3)
    by_head(raws // 3, raws * 2 // 3)
    part2(3)
    by_head(raws * 2 // 3, raws)
    put_raw(raws - 2).wait()
    put_raw(raws - 1).wait()

    def layer(l, carry):
        def loop(count, step):
            def body(i, inner):
                step(l, i)
                return inner

            lax.fori_loop(0, count, body, 0)

        @pl.when(l > 0)
        def _():
            layer_norms(l, 0, seq // norm_rows)

        loop(n_b, up_step)
        loop(n_a, head_step)
        loop(n_c, down_step)
        return carry

    lax.fori_loop(0, num_layers, layer, 0)
    for k in range(chunks - 3, chunks):
        wait_sent(k)


def solution(mesh):
    row_spec = P(("dp", "fsdp"), None, None)
    in_specs = (row_spec, P(("dp", "fsdp")), P(None, None, "fsdp"), P(None, "fsdp", None, None), P(None, "fsdp"),
                P(None, "fsdp", None), P(None, "fsdp"), P(None, "fsdp", None), P(None, "fsdp"), P(None, "fsdp", None),
                P(None, "fsdp"))
    n = mesh.shape["fsdp"]
    assert n % 2 == 0 and mesh.shape["dp"] % 2 == 0

    def local_step(hidden, lens, ln_par, w_qkv, b_qkv, w_out, b_out, w_up, b_up, w_down, b_down):
        _, seq, d_model = hidden.shape
        num_layers, tile, heads, triple = w_qkv.shape
        rps = w_down.shape[1] // tile
        assert hidden.shape[0] == 1 and n == 8 and n * tile == d_model and triple == 3 * tile and heads == n
        assert n * rps // 2 + 2 * (d_model // tile) == n * rps
        rot_half = tile // 8
        wide = 128
        raw_rows = 32 * heads
        dims = (n, num_layers, heads, tile, seq, d_model, rps, rot_half)
        chunks = num_layers * (heads + n * rps // 2 + d_model // tile)
        ring = n // 2
        vmem = pl.BlockSpec(memory_space=pltpu.VMEM)
        anywhere = pl.BlockSpec(memory_space=pl.ANY)
        dma = pltpu.SemaphoreType.DMA
        smalls = (ln_par, b_qkv, b_out, b_up, b_down)
        out, _, _ = pl.pallas_call(
            functools.partial(kernel, dims),
            name="layers",
            out_shape=(pltpu.VMEM((seq, d_model), BF16),
                       jax.ShapeDtypeStruct((chunks, 3, n, tile, tile), BF16),
                       jax.ShapeDtypeStruct((num_layers, heads, tile, triple), BF16)),
            in_specs=[anywhere, pl.BlockSpec(memory_space=pltpu.SMEM)] + [vmem] * 5 + [anywhere] * 4,
            out_specs=(vmem, anywhere, anywhere),
            scratch_shapes=[
                pltpu.VMEM((seq, d_model), BF16),
                pltpu.VMEM((seq, d_model), BF16),
                pltpu.VMEM((seq, d_model), BF16),
                pltpu.VMEM((rps, seq, d_model), BF16),
                pltpu.VMEM((seq, d_model), F32),
                pltpu.VMEM((seq, tile), BF16),
                pltpu.VMEM((seq, tile), BF16),
                pltpu.VMEM((seq, tile), BF16),
                pltpu.VMEM((2, 4, d_model, tile), BF16),
                pltpu.VMEM((3, seq, wide), F32),
                *[pltpu.VMEM((n,) + p.shape, p.dtype) for p in smalls],
                pltpu.VMEM((n, num_layers, 16, tile), F32),
                pltpu.VMEM((2, raw_rows, triple), BF16),
                pltpu.VMEM((raw_rows * triple // wide, wide), F32),
                pltpu.VMEM((2, heads, raw_rows // heads, triple), BF16),
                dma((SLOTS,)),
                dma((SLOTS, 3)),
                dma((SLOTS, 3)),
                dma((SLOTS, 3)),
                dma((SLOTS, 3)),
                dma((2, 4)),
                dma((5,)),
                dma((5,)),
                dma((2,)),
                dma((2,)),
                dma,
            ],
            compiler_params=pltpu.CompilerParams(
                collective_id=0, has_side_effects=True, vmem_limit_bytes=59 * 2**20),
        )(hidden.reshape(seq, d_model), lens, *smalls,
          w_qkv.reshape(num_layers, tile * heads, triple), w_out, w_up, w_down)
        return out.reshape(1, seq, d_model)

    return jax.shard_map(local_step, mesh=mesh, in_specs=in_specs, out_specs=row_spec, check_vma=False)
```

```python
import functools

import jax
import jax.numpy as jnp
import numpy as np
from jax import lax
from jax.experimental import pallas as pl
from jax.experimental.pallas import tpu as pltpu
from jax.sharding import PartitionSpec as P

ROPE_BASE = 10000.0
LN_EPS = 1e-5
MESH = pl.DeviceIdType.MESH
SLOTS = 16
LATE = 4
ROWS = 256
DOT_ROWS = 256
F32 = jnp.float32
BF16 = jnp.bfloat16


def rope_row(rot_dim, width):
    inv_freq = np.float32(1.0) / (np.float32(ROPE_BASE) ** (np.arange(0, rot_dim, 2, dtype=np.float32) / np.float32(rot_dim)))
    lane = lax.broadcasted_iota(jnp.int32, (1, width), 1)
    row = jnp.zeros((1, width), F32)
    for i, value in enumerate(inv_freq):
        row = jnp.where((lane == i) | (lane == i + rot_dim // 2), float(value), row)
    return row


def kernel(dims, hid, lens, ln_own, bq_own, bo_own, bu_own, bd_own, wq_raw, wo, wu, wd, xs, gath, wq, a_s, m_s, ctx,
           act, acc, q_s, k_s, v_s, wbuf, tabs, ln_g, bq_g, bo_g, bu_g, bd_g, bias, raw, raw32, turned, send, rs, ls, ysem, dd,
           ld, small_send, small_recv, raw_in, raw_out, io_sem):
    n, num_layers, heads, tile, seq, d_model, rps, rot_half = dims
    ring = n // 2
    n_a, n_b, n_c = heads, n * rps // 2, d_model // tile
    per_layer = n_a + n_b + n_c
    chunks = num_layers * per_layer
    wide = tabs.shape[2]
    scale = float(tile) ** -0.5

    d, f = lax.axis_index("dp"), lax.axis_index("fsdp")
    x, c = f // 2, f % 2
    par = d % 2
    right = ((x + 1) % ring) * 2 + c
    left = ((x + ring - 1) % ring) * 2 + c
    far = ((x + 2) % ring) * 2 + c
    sib = x * 2 + 1 - c
    mate = d + 1 - 2 * par
    mine, other = 2 * par, 2 - 2 * par

    def remote(src, dst, s_sem, r_sem, where):
        return pltpu.make_async_remote_copy(
            src_ref=src, dst_ref=dst, send_sem=s_sem, recv_sem=r_sem, device_id=where, device_id_type=MESH)

    to_right, to_left, to_sib, to_mate = {"fsdp": right}, {"fsdp": left}, {"fsdp": sib}, {"dp": mate}

    def q_tile(l, h, i):
        return wq.at[l, h, :, pl.ds(i * tile, tile) if isinstance(i, int) else pl.ds(pl.multiple_of(i * tile, tile), tile)]

    def up_tile(l, u):
        return wu.at[l, :, pl.ds(pl.multiple_of((u % n) * (rps * tile) + (u // n) * tile, tile), tile)]

    def down_tile(l, v):
        return wd.at[l, pl.ds(pl.multiple_of((v // n_c) * tile, tile), tile),
                     pl.ds(pl.multiple_of((v % n_c) * tile, tile), tile)]

    def out_tile(l, j):
        return wo.at[l, :, pl.ds(pl.multiple_of(j * tile, tile), tile)]

    def with_own(k, go):
        l, r = k // per_layer, k % per_layer

        @pl.when(r < n_b)
        def _():
            go(lambda i: down_tile(l, r) if isinstance(i, int) and i == 1 else up_tile(l, 2 * r + i // 2))

        @pl.when((r >= n_b) & (r < n_b + n_a))
        def _():
            go(lambda i: q_tile(l, r - n_b, i))

        @pl.when(r >= n_a + n_b)
        def _():
            j = r - n_a - n_b
            go(lambda i: out_tile(l, j) if isinstance(i, int) and i == 1 else down_tile(l, n_b + 2 * j + i // 2))

    def own_first(k):
        slot = k % SLOTS

        def go(own):
            remote(own(mine), gath.at[k, mine, f], send.at[slot], rs.at[slot, 0], to_right).start()
            remote(own(1), gath.at[k, 1, f], send.at[slot], ls.at[slot, 0], to_left).start()
            for role, i in enumerate((mine, 1)):
                remote(own(i), gath.at[k, i, f], send.at[slot], dd.at[slot, role], to_sib).start()

        with_own(k, go)

    def own_second(k):
        slot = k % SLOTS

        def go(own):
            remote(own(1), gath.at[k, 1, f], send.at[slot], rs.at[slot, 1], to_right).start()
            remote(own(mine), gath.at[k, mine, f], send.at[slot], ls.at[slot, 1], to_left).start()
            remote(own(other), gath.at[k, other, f], send.at[slot], dd.at[slot, 2], to_sib).start()

        with_own(k, go)

    def wait_tile(sem):
        ref = gath.at[0, 0, 0]
        pltpu.make_async_copy(ref, ref, sem).wait()

    def pass_on(k, i, s, sem, where):
        t = gath.at[k, i, s]
        remote(t, t, send.at[k % SLOTS], sem, where).start()

    def from_sides(k):
        slot = k % SLOTS
        wait_tile(rs.at[slot, 0])
        pass_on(k, mine, left, rs.at[slot, 2], to_right)
        pass_on(k, mine, left, ysem.at[slot, 0], to_mate)
        pass_on(k, mine, left, dd.at[slot, 0], to_sib)
        wait_tile(ls.at[slot, 0])
        pass_on(k, 1, right, ls.at[slot, 2], to_left)
        pass_on(k, 1, right, dd.at[slot, 1], to_sib)

    def from_sides_again(k):
        slot = k % SLOTS
        wait_tile(ls.at[slot, 1])
        pass_on(k, mine, right, ysem.at[slot, 1], to_mate)
        pass_on(k, mine, right, dd.at[slot, 0], to_sib)
        wait_tile(rs.at[slot, 1])
        pass_on(k, 1, left, dd.at[slot, 1], to_sib)

    def from_far(k):
        slot = k % SLOTS
        wait_tile(rs.at[slot, 2])
        pass_on(k, mine, far, ysem.at[slot, 2], to_mate)
        pass_on(k, mine, far, dd.at[slot, 0], to_sib)
        wait_tile(ls.at[slot, 2])
        pass_on(k, 1, far, dd.at[slot, 1], to_sib)

    def from_mate(i, s):
        def do(k):
            slot = k % SLOTS
            wait_tile(ysem.at[slot, i])
            pass_on(k, other, s, dd.at[slot, 2], to_sib)

        return do

    sent_tiles = 3 * (ring - 1) + 3 * ring

    def wait_sib(k, role):
        ref = gath.at[0, 0, pl.ds(0, ring)]
        pltpu.make_async_copy(ref, ref, dd.at[k % SLOTS, role]).wait()

    def wait_sent(k):
        ref = gath.at[0, :, pl.ds(0, sent_tiles // 3)]
        pltpu.make_async_copy(ref, ref, send.at[k % SLOTS]).wait()

    def load_tile(k, kk, i, to, own):
        slot = k % 2
        for step in range(1, n):
            s = (f + step) % n
            pltpu.make_async_copy(
                gath.at[kk, i, s], wbuf.at[slot, to, pl.ds(pl.multiple_of(s * tile, tile), tile)], ld.at[slot, to]).start()
        pltpu.make_async_copy(own, wbuf.at[slot, to, pl.ds(pl.multiple_of(f * tile, tile), tile)], ld.at[slot, to]).start()

    def load_down(k, i):
        j = k % per_layer - n_a - n_b
        load_tile(k, k, i, i, down_tile(k // per_layer, n_b + 2 * j + i // 2))

    def load(k):
        l, r = k // per_layer, k % per_layer
        for role in range(3):
            wait_sib(k, role)

        @pl.when(r < n_b)
        def _():
            for i in (0, 2):
                load_tile(k, k, i, i, up_tile(l, 2 * r + i // 2))

        @pl.when((r >= LATE) & (r < n_b))
        def _():
            load_tile(k, k - LATE, 1, 3, down_tile(l, r - LATE))

        @pl.when(r >= n_b)
        def _():
            for i in range(3):
                load_tile(k, k, i, i, q_tile(l, r - n_b, i))

    def load_first(k):
        l, j = k // per_layer, k % per_layer - n_a - n_b
        for role in range(2):
            wait_sib(k, role)
        load_tile(k, k, 1, 1, out_tile(l, j))
        load_down(k, mine)

        @pl.when(j < LATE)
        def _():
            load_tile(k, k - n_a - LATE, 1, 3, down_tile(l, n_b - LATE + j))

    def load_last(k):
        wait_sib(k, 2)
        load_down(k, other)

    def loaded(slot, to):
        pltpu.make_async_copy(wbuf.at[slot, to], wbuf.at[slot, to], ld.at[slot, to]).wait()

    def within(k, do, phases=None):
        r = k % per_layer
        these = {None: True, "first": r < n_a + n_b, "last": r >= n_a + n_b}[phases]

        @pl.when((k >= 0) & (k < chunks) & these)
        def _():
            do(k)

    def part0(t):
        within(t - 7, wait_sent)
        within(t, own_first)
        within(t - 1, from_sides)
        within(t - 4, from_mate(2, far), "last")

    def part1(t):
        within(t - 2, from_far)
        within(t - 3, from_mate(1, right))
        within(t - 3, from_mate(2, far), "first")
        within(t - 4, load_last, "last")

    def part2(t):
        within(t, own_second)
        within(t - 1, from_sides_again)
        within(t - 2, from_mate(0, left))
        within(t - 2, load_first, "last")
        within(t - 3, load, "first")

    blocks = seq // ROWS

    def rows_of(b):
        return pl.ds(b * ROWS, ROWS)

    dot_blocks = [pl.ds(b * DOT_ROWS, DOT_ROWS) for b in range(seq // DOT_ROWS)]

    def cols_of(j):
        return pl.ds(pl.multiple_of(j * tile, tile), tile)

    def row(s, l, i):
        return bias[s, l, pl.ds(i, 1), :]

    def ln_row(s, l, i):
        return ln_g[s, l, pl.ds(i, 1), :]

    norm_rows = 128

    def layer_norms(l, first, last):
        step = norm_rows

        def body(b, carry):
            rows = pl.ds(pl.multiple_of(b * step, step), step)
            v = xs[rows, :].astype(F32)
            cen = v - jnp.mean(v, axis=-1, keepdims=True)
            inv = lax.rsqrt(jnp.mean(cen * cen, axis=-1, keepdims=True) + LN_EPS)
            for s in range(n):
                cols = pl.ds(s * tile, tile)
                norm = cen[:, s * tile:(s + 1) * tile] * inv
                a_s[rows, cols] = (norm * ln_row(s, l, 0) + ln_row(s, l, 1)).astype(BF16)
                m_s[rows, cols] = (norm * ln_row(s, l, 2) + ln_row(s, l, 3)).astype(BF16)
                acc[rows, cols] = v[:, s * tile:(s + 1) * tile] + (row(s, l, 3) + row(s, l, 4 + rps))
            return carry

        lax.fori_loop(first, last, body, 0)

    def dot(lhs, slot, to):
        return jnp.dot(lhs, wbuf[slot, to], preferred_element_type=F32)

    def rotate(v, rows):
        u = v[:, :wide].astype(F32)
        turned = (u * tabs[0, rows, :] + pltpu.roll(u, wide - rot_half, 1) * tabs[1, rows, :]
                  + pltpu.roll(u, rot_half, 1) * tabs[2, rows, :])
        return turned.astype(BF16)

    def project(l, h, slot, i, ref):
        for rows in dot_blocks:
            v = (dot(a_s[rows, :], slot, i) + row(h, l, i)).astype(BF16)
            if i < 2:
                ref[rows, pl.ds(0, wide)] = rotate(v, rows)
                ref[rows, pl.ds(wide, tile - wide)] = v[:, wide:]
            else:
                ref[rows, :] = v

    def attend(h, b):
        width = (b + 1) * ROWS
        s = lax.dot_general(q_s[rows_of(b), :], k_s[pl.ds(0, width), :], (((1,), (1,)), ((), ())),
                            preferred_element_type=F32) * scale
        col = lax.broadcasted_iota(jnp.int32, (ROWS, width), 1)
        at = lax.broadcasted_iota(jnp.int32, (ROWS, width), 0) + b * ROWS
        s = jnp.where((col <= at) & (col < lens[0]), s, -1e30)
        e = jnp.exp(s - jnp.max(s, axis=-1, keepdims=True))
        p = (e * (1.0 / jnp.sum(e, axis=-1, keepdims=True))).astype(BF16)
        ctx[rows_of(b), cols_of(h)] = jnp.dot(p, v_s[pl.ds(0, width), :], preferred_element_type=F32).astype(BF16)

    def up(l, u, slot, to):
        s, rp = u % n, u // n
        for rows in dot_blocks:
            v = dot(m_s[rows, :], slot, to) + row(s, l, 4 + rp)
            g = (0.5 * v) * (1.0 + lax.erf(v * (0.5 ** 0.5)))
            act[rp, rows, cols_of(s)] = g.astype(BF16)

    def add_to(j, slot, to, lhs):
        for rows in dot_blocks:
            acc[rows, cols_of(j)] += dot(lhs(rows), slot, to)

    def down(v, slot, to):
        add_to(v % n_c, slot, to, lambda rows: act[v // n_c, rows, :])

    def head_step(l, h):
        k = l * per_layer + n_b + h
        slot = k % 2
        part0(k + 4)
        loaded(slot, 0)
        loaded(slot, 1)
        project(l, h, slot, 0, q_s)
        project(l, h, slot, 1, k_s)
        part1(k + 4)
        loaded(slot, 2)
        project(l, h, slot, 2, v_s)
        for b in range(blocks // 2):
            attend(h, b)
        part2(k + 4)
        for b in range(blocks // 2, blocks):
            attend(h, b)

        @pl.when(h == n_a - 1)
        def _():
            out_now(0, 1 - slot)

    def up_step(l, j):
        k = l * per_layer + j
        slot = k % 2
        part0(k + 4)
        loaded(slot, 0)
        up(l, 2 * j, slot, 0)
        part1(k + 4)
        loaded(slot, 2)
        up(l, 2 * j + 1, slot, 2)
        part2(k + 4)

        @pl.when(j >= LATE)
        def _():
            loaded(slot, 3)
            down(j - LATE, slot, 3)

    def out_now(j, slot):
        loaded(slot, 1)
        add_to(j, slot, 1, lambda rows: ctx[rows, :])

    def down_now(j, slot, i):
        loaded(slot, i)
        down(n_b + 2 * j + i // 2, slot, i)

    def down_step(l, j):
        k = l * per_layer + n_a + n_b + j
        slot = k % 2
        part0(k + 4)

        @pl.when(j == 0)
        def _():
            down_now(j, slot, mine)

        @pl.when(j < n_c - 1)
        def _():
            out_now(j + 1, 1 - slot)

        part1(k + 4)

        @pl.when(j < n_c - 1)
        def _():
            down_now(j + 1, 1 - slot, mine)

        @pl.when(j < LATE)
        def _():
            loaded(slot, 3)
            down(n_b - LATE + j, slot, 3)

        part2(k + 4)
        down_now(j, slot, other)

        @pl.when(j >= n_c // 2)
        def _():
            cols = pl.ds(pl.multiple_of((2 * j - n_c) * tile, 2 * tile), 2 * tile)
            for b in range(blocks):
                xs[rows_of(b), cols] = acc[rows_of(b), cols].astype(BF16)

    def rotary_tables():
        freq = rope_row(2 * rot_half, wide)
        for b in range(blocks):
            at = (lax.broadcasted_iota(jnp.int32, (ROWS, wide), 0) + b * ROWS).astype(F32)
            lane = lax.broadcasted_iota(jnp.int32, (ROWS, wide), 1)
            angle = at * freq
            cos, sin = jnp.cos(angle), jnp.sin(angle)
            tabs[0, rows_of(b), :] = jnp.where(lane < 2 * rot_half, cos, 1.0)
            tabs[1, rows_of(b), :] = jnp.where(lane < rot_half, -sin, 0.0)
            tabs[2, rows_of(b), :] = jnp.where((lane >= rot_half) & (lane < 2 * rot_half), sin, 0.0)

    raw_rows = raw.shape[1]
    per_raw = tile * heads // raw_rows
    raws = num_layers * per_raw

    def get_raw(b):
        return pltpu.make_async_copy(
            wq_raw.at[b // per_raw, pl.ds(pl.multiple_of((b % per_raw) * raw_rows, raw_rows), raw_rows)],
            raw.at[b % 2], raw_in.at[b % 2])

    def put_raw(b):
        some = raw_rows // heads
        return pltpu.make_async_copy(
            turned.at[b % 2], wq.at[b // per_raw, :, pl.ds(pl.multiple_of((b % per_raw) * some, some), some)],
            raw_out.at[b % 2])

    def by_head(first, last):
        def body(b, carry):
            get_raw(b).wait()
            for q in range(raw.shape[2] // wide):
                raw32[pl.ds(q * raw_rows, raw_rows), :] = raw[b % 2, :, pl.ds(q * wide, wide)].astype(F32)

            @pl.when(b + 2 < raws)
            def _():
                get_raw(b + 2).start()

            @pl.when(b >= 2)
            def _():
                put_raw(b - 2).wait()

            for h in range(heads):
                for q in range(raw.shape[2] // wide):
                    turned[b % 2, h, :, pl.ds(q * wide, wide)] = (
                        raw32[pl.ds(q * raw_rows + h, raw_rows // heads, stride=heads), :].astype(BF16))
            put_raw(b).start()
            return carry

        lax.fori_loop(first, last, body, 0)

    def unpack_biases():
        for s in range(n):
            for g, at, count in ((bq_g, 0, 3), (bo_g, 3, 1), (bu_g, 4, rps), (bd_g, 4 + rps, 1)):
                for i in range(count):
                    v = g[s, :, pl.ds(i * tile, tile)].astype(F32)
                    for l in range(num_layers):
                        bias[s, l, pl.ds(at + i, 1), :] = v[l:l + 1]

    get_hidden = pltpu.make_async_copy(hid, xs, io_sem)
    get_hidden.start()
    get_raw(0).start()
    get_raw(1).start()
    barrier = pltpu.get_barrier_semaphore()
    for step in range(1, n):
        pl.semaphore_signal(barrier, inc=1, device_id={"fsdp": (f + step) % n}, device_id_type=MESH)
    pl.semaphore_signal(barrier, inc=1, device_id=to_mate, device_id_type=MESH)
    pl.semaphore_wait(barrier, n)

    smalls = ((ln_own, ln_g), (bq_own, bq_g), (bo_own, bo_g), (bu_own, bu_g), (bd_own, bd_g))
    own_first(0)
    for i, (own, everyone) in enumerate(smalls):
        for step in range(1, n):
            remote(own, everyone.at[f], small_send.at[i], small_recv.at[i], {"fsdp": (f + step) % n}).start()
    own_second(0)
    for own, everyone in smalls:
        everyone[f] = own[...]
    rotary_tables()
    part0(1)
    for i, (own, everyone) in enumerate(smalls):
        ref = everyone.at[pl.ds(0, n - 1)]
        pltpu.make_async_copy(ref, ref, small_send.at[i]).wait()
        pltpu.make_async_copy(ref, ref, small_recv.at[i]).wait()
    unpack_biases()
    part1(1)
    part2(1)
    get_hidden.wait()
    norms = seq // norm_rows
    for i, part in enumerate((part0, part1, part2, part0)):
        layer_norms(0, norms * i // 4, norms * (i + 1) // 4)
        part(2 + i // 3)
    by_head(0, raws // 3)
    part1(3)
    by_head(raws // 3, raws * 2 // 3)
    part2(3)
    by_head(raws * 2 // 3, raws)
    put_raw(raws - 2).wait()
    put_raw(raws - 1).wait()

    def layer(l, carry):
        def loop(count, step):
            def body(i, inner):
                step(l, i)
                return inner

            lax.fori_loop(0, count, body, 0)

        @pl.when(l > 0)
        def _():
            layer_norms(l, 0, seq // norm_rows)

        loop(n_b, up_step)
        loop(n_a, head_step)
        loop(n_c, down_step)
        return carry

    lax.fori_loop(0, num_layers, layer, 0)
    for k in range(chunks - 3, chunks):
        wait_sent(k)


def solution(mesh):
    row_spec = P(("dp", "fsdp"), None, None)
    in_specs = (row_spec, P(("dp", "fsdp")), P(None, None, "fsdp"), P(None, "fsdp", None, None), P(None, "fsdp"),
                P(None, "fsdp", None), P(None, "fsdp"), P(None, "fsdp", None), P(None, "fsdp"), P(None, "fsdp", None),
                P(None, "fsdp"))
    n = mesh.shape["fsdp"]
    assert n % 2 == 0 and mesh.shape["dp"] % 2 == 0

    def local_step(hidden, lens, ln_par, w_qkv, b_qkv, w_out, b_out, w_up, b_up, w_down, b_down):
        _, seq, d_model = hidden.shape
        num_layers, tile, heads, triple = w_qkv.shape
        rps = w_down.shape[1] // tile
        assert hidden.shape[0] == 1 and n == 8 and n * tile == d_model and triple == 3 * tile and heads == n
        assert n * rps // 2 + 2 * (d_model // tile) == n * rps
        rot_half = tile // 8
        wide = 128
        raw_rows = 32 * heads
        dims = (n, num_layers, heads, tile, seq, d_model, rps, rot_half)
        chunks = num_layers * (heads + n * rps // 2 + d_model // tile)
        ring = n // 2
        vmem = pl.BlockSpec(memory_space=pltpu.VMEM)
        anywhere = pl.BlockSpec(memory_space=pl.ANY)
        dma = pltpu.SemaphoreType.DMA
        smalls = (ln_par, b_qkv, b_out, b_up, b_down)
        out, _, _ = pl.pallas_call(
            functools.partial(kernel, dims),
            name="layers",
            out_shape=(pltpu.VMEM((seq, d_model), BF16),
                       jax.ShapeDtypeStruct((chunks, 3, n, tile, tile), BF16),
                       jax.ShapeDtypeStruct((num_layers, heads, tile, triple), BF16)),
            in_specs=[anywhere, pl.BlockSpec(memory_space=pltpu.SMEM)] + [vmem] * 5 + [anywhere] * 4,
            out_specs=(vmem, anywhere, anywhere),
            scratch_shapes=[
                pltpu.VMEM((seq, d_model), BF16),
                pltpu.VMEM((seq, d_model), BF16),
                pltpu.VMEM((seq, d_model), BF16),
                pltpu.VMEM((rps, seq, d_model), BF16),
                pltpu.VMEM((seq, d_model), F32),
                pltpu.VMEM((seq, tile), BF16),
                pltpu.VMEM((seq, tile), BF16),
                pltpu.VMEM((seq, tile), BF16),
                pltpu.VMEM((2, 4, d_model, tile), BF16),
                pltpu.VMEM((3, seq, wide), F32),
                *[pltpu.VMEM((n,) + p.shape, p.dtype) for p in smalls],
                pltpu.VMEM((n, num_layers, 16, tile), F32),
                pltpu.VMEM((2, raw_rows, triple), BF16),
                pltpu.VMEM((raw_rows * triple // wide, wide), F32),
                pltpu.VMEM((2, heads, raw_rows // heads, triple), BF16),
                dma((SLOTS,)),
                dma((SLOTS, 3)),
                dma((SLOTS, 3)),
                dma((SLOTS, 3)),
                dma((SLOTS, 3)),
                dma((2, 4)),
                dma((5,)),
                dma((5,)),
                dma((2,)),
                dma((2,)),
                dma,
            ],
            compiler_params=pltpu.CompilerParams(
                collective_id=0, has_side_effects=True, vmem_limit_bytes=59 * 2**20),
        )(hidden.reshape(seq, d_model), lens, *smalls,
          w_qkv.reshape(num_layers, tile * heads, triple), w_out, w_up, w_down)
        return out.reshape(1, seq, d_model)

    return jax.shard_map(local_step, mesh=mesh, in_specs=in_specs, out_specs=row_spec, check_vma=False)
```

```python
import functools

import jax
import jax.numpy as jnp
import numpy as np
from jax import lax
from jax.experimental import pallas as pl
from jax.experimental.pallas import tpu as pltpu
from jax.sharding import PartitionSpec as P

ROPE_BASE = 10000.0
LN_EPS = 1e-5
MESH = pl.DeviceIdType.MESH
SLOTS = 16
LATE = 4
ROWS = 256
DOT_ROWS = 256
F32 = jnp.float32
BF16 = jnp.bfloat16


def rope_row(rot_dim, width):
    inv_freq = np.float32(1.0) / (np.float32(ROPE_BASE) ** (np.arange(0, rot_dim, 2, dtype=np.float32) / np.float32(rot_dim)))
    lane = lax.broadcasted_iota(jnp.int32, (1, width), 1)
    row = jnp.zeros((1, width), F32)
    for i, value in enumerate(inv_freq):
        row = jnp.where((lane == i) | (lane == i + rot_dim // 2), float(value), row)
    return row


def kernel(dims, hid, lens_own, ln_own, bq_own, bo_own, bu_own, bd_own, wq_raw, wo, wu, wd, xs, gath, wq, a_s, m_s, ctx,
           act, acc, q_s, k_s, v_s, wbuf, tabs, lens, ln_g, bq_g, bo_g, bu_g, bd_g, bias, raw, raw32, turned, send, rs, ls, ysem, dd,
           ld, small_send, small_recv, small_own, raw_in, raw_out, io_sem):
    n, num_layers, heads, tile, seq, d_model, rps, rot_half = dims
    ring = n // 2
    n_a, n_b, n_c = heads, n * rps // 2, d_model // tile
    per_layer = n_a + n_b + n_c
    chunks = num_layers * per_layer
    wide = tabs.shape[2]
    scale = float(tile) ** -0.5

    d, f = lax.axis_index("dp"), lax.axis_index("fsdp")
    x, c = f // 2, f % 2
    par = d % 2
    right = ((x + 1) % ring) * 2 + c
    left = ((x + ring - 1) % ring) * 2 + c
    far = ((x + 2) % ring) * 2 + c
    sib = x * 2 + 1 - c
    mate = d + 1 - 2 * par
    mine, other = 2 * par, 2 - 2 * par

    def remote(src, dst, s_sem, r_sem, where):
        return pltpu.make_async_remote_copy(
            src_ref=src, dst_ref=dst, send_sem=s_sem, recv_sem=r_sem, device_id=where, device_id_type=MESH)

    to_right, to_left, to_sib, to_mate = {"fsdp": right}, {"fsdp": left}, {"fsdp": sib}, {"dp": mate}

    def q_tile(l, h, i):
        return wq.at[l, h, :, pl.ds(i * tile, tile) if isinstance(i, int) else pl.ds(pl.multiple_of(i * tile, tile), tile)]

    def up_tile(l, u):
        return wu.at[l, :, pl.ds(pl.multiple_of((u % n) * (rps * tile) + (u // n) * tile, tile), tile)]

    def down_tile(l, v):
        return wd.at[l, pl.ds(pl.multiple_of((v // n_c) * tile, tile), tile),
                     pl.ds(pl.multiple_of((v % n_c) * tile, tile), tile)]

    def out_tile(l, j):
        return wo.at[l, :, pl.ds(pl.multiple_of(j * tile, tile), tile)]

    def with_own(k, go):
        l, r = k // per_layer, k % per_layer

        @pl.when(r < n_b)
        def _():
            go(lambda i: down_tile(l, r) if isinstance(i, int) and i == 1 else up_tile(l, 2 * r + i // 2))

        @pl.when((r >= n_b) & (r < n_b + n_a))
        def _():
            go(lambda i: q_tile(l, r - n_b, i))

        @pl.when(r >= n_a + n_b)
        def _():
            j = r - n_a - n_b
            go(lambda i: out_tile(l, j) if isinstance(i, int) and i == 1 else down_tile(l, n_b + 2 * j + i // 2))

    def own_first(k):
        slot = k % SLOTS
        at_once = isinstance(k, int)

        def go(own):
            remote(own(mine), gath.at[k, mine, f], send.at[slot], rs.at[slot, 0], to_right).start()
            if at_once:
                remote(own(mine), gath.at[k, mine, f], send.at[slot], ls.at[slot, 1], to_left).start()
            else:
                remote(own(1), gath.at[k, 1, f], send.at[slot], ls.at[slot, 0], to_left).start()
            for role, i in enumerate((mine, 1)):
                remote(own(i), gath.at[k, i, f], send.at[slot], dd.at[slot, role], to_sib).start()

        with_own(k, go)

    def own_second(k):
        slot = k % SLOTS
        at_once = isinstance(k, int)

        def go(own):
            remote(own(1), gath.at[k, 1, f], send.at[slot], rs.at[slot, 1], to_right).start()
            if at_once:
                remote(own(1), gath.at[k, 1, f], send.at[slot], ls.at[slot, 0], to_left).start()
            else:
                remote(own(mine), gath.at[k, mine, f], send.at[slot], ls.at[slot, 1], to_left).start()
            remote(own(other), gath.at[k, other, f], send.at[slot], dd.at[slot, 2], to_sib).start()

        with_own(k, go)

    def wait_tile(sem):
        ref = gath.at[0, 0, 0]
        pltpu.make_async_copy(ref, ref, sem).wait()

    def pass_on(k, i, s, sem, where):
        t = gath.at[k, i, s]
        remote(t, t, send.at[k % SLOTS], sem, where).start()

    def left_mine(k):
        slot = k % SLOTS
        wait_tile(rs.at[slot, 0])
        pass_on(k, mine, left, rs.at[slot, 2], to_right)
        pass_on(k, mine, left, ysem.at[slot, 0], to_mate)
        pass_on(k, mine, left, dd.at[slot, 0], to_sib)

    def right_one(k):
        slot = k % SLOTS
        wait_tile(ls.at[slot, 0])
        pass_on(k, 1, right, ls.at[slot, 2], to_left)
        pass_on(k, 1, right, dd.at[slot, 1], to_sib)

    def right_mine(k):
        slot = k % SLOTS
        wait_tile(ls.at[slot, 1])
        pass_on(k, mine, right, ysem.at[slot, 1], to_mate)
        pass_on(k, mine, right, dd.at[slot, 0], to_sib)

    def left_one(k):
        slot = k % SLOTS
        wait_tile(rs.at[slot, 1])
        pass_on(k, 1, left, dd.at[slot, 1], to_sib)

    def from_sides(k):
        left_mine(k)
        right_one(k)

    def from_sides_again(k):
        right_mine(k)
        left_one(k)

    def from_far(k):
        slot = k % SLOTS
        wait_tile(rs.at[slot, 2])
        pass_on(k, mine, far, ysem.at[slot, 2], to_mate)
        pass_on(k, mine, far, dd.at[slot, 0], to_sib)
        wait_tile(ls.at[slot, 2])
        pass_on(k, 1, far, dd.at[slot, 1], to_sib)

    def from_mate(i, s):
        def do(k):
            slot = k % SLOTS
            wait_tile(ysem.at[slot, i])
            pass_on(k, other, s, dd.at[slot, 2], to_sib)

        return do

    sent_tiles = 3 * (ring - 1) + 3 * ring

    def wait_sib(k, role):
        ref = gath.at[0, 0, pl.ds(0, ring)]
        pltpu.make_async_copy(ref, ref, dd.at[k % SLOTS, role]).wait()

    def wait_sent(k):
        ref = gath.at[0, :, pl.ds(0, sent_tiles // 3)]
        pltpu.make_async_copy(ref, ref, send.at[k % SLOTS]).wait()

    def load_tile(k, kk, i, to, own):
        slot = k % 2
        for step in range(1, n):
            s = (f + step) % n
            pltpu.make_async_copy(
                gath.at[kk, i, s], wbuf.at[slot, to, pl.ds(pl.multiple_of(s * tile, tile), tile)], ld.at[slot, to]).start()
        pltpu.make_async_copy(own, wbuf.at[slot, to, pl.ds(pl.multiple_of(f * tile, tile), tile)], ld.at[slot, to]).start()

    def load_down(k, i):
        j = k % per_layer - n_a - n_b
        load_tile(k, k, i, i, down_tile(k // per_layer, n_b + 2 * j + i // 2))

    def load(k):
        l, r = k // per_layer, k % per_layer
        for role in range(3):
            wait_sib(k, role)

        @pl.when(r < n_b)
        def _():
            for i in (0, 2):
                load_tile(k, k, i, i, up_tile(l, 2 * r + i // 2))

        @pl.when((r >= LATE) & (r < n_b))
        def _():
            load_tile(k, k - LATE, 1, 3, down_tile(l, r - LATE))

        @pl.when(r >= n_b)
        def _():
            for i in range(3):
                load_tile(k, k, i, i, q_tile(l, r - n_b, i))

    def load_first(k):
        l, j = k // per_layer, k % per_layer - n_a - n_b
        for role in range(2):
            wait_sib(k, role)
        load_tile(k, k, 1, 1, out_tile(l, j))
        load_down(k, mine)

        @pl.when(j < LATE)
        def _():
            load_tile(k, k - n_a - LATE, 1, 3, down_tile(l, n_b - LATE + j))

    def load_last(k):
        wait_sib(k, 2)
        load_down(k, other)

    def loaded(slot, to):
        pltpu.make_async_copy(wbuf.at[slot, to], wbuf.at[slot, to], ld.at[slot, to]).wait()

    def within(k, do, phases=None):
        r = k % per_layer
        these = {None: True, "first": r < n_a + n_b, "last": r >= n_a + n_b}[phases]

        @pl.when((k >= 0) & (k < chunks) & these)
        def _():
            do(k)

    def part0(t):
        within(t - 7, wait_sent)
        within(t, own_first)
        within(t - 1, from_sides)
        within(t - 4, from_mate(2, far), "last")

    def part1(t):
        within(t - 2, from_far)
        within(t - 3, from_mate(1, right))
        within(t - 3, from_mate(2, far), "first")
        within(t - 4, load_last, "last")

    def part2(t):
        within(t, own_second)
        within(t - 1, from_sides_again)
        within(t - 2, from_mate(0, left))
        within(t - 2, load_first, "last")
        within(t - 3, load, "first")

    blocks = seq // ROWS

    def rows_of(b):
        return pl.ds(b * ROWS, ROWS)

    dot_blocks = [pl.ds(b * DOT_ROWS, DOT_ROWS) for b in range(seq // DOT_ROWS)]

    def cols_of(j):
        return pl.ds(pl.multiple_of(j * tile, tile), tile)

    def row(s, l, i):
        return bias[s, l, pl.ds(i, 1), :]

    def ln_row(s, l, i):
        return ln_g[s, l, pl.ds(i, 1), :]

    norm_rows = 128

    def layer_norms(l, first, last):
        step = norm_rows

        def body(b, carry):
            rows = pl.ds(pl.multiple_of(b * step, step), step)
            v = xs[rows, :].astype(F32)
            cen = v - jnp.mean(v, axis=-1, keepdims=True)
            inv = lax.rsqrt(jnp.mean(cen * cen, axis=-1, keepdims=True) + LN_EPS)
            for s in range(n):
                cols = pl.ds(s * tile, tile)
                norm = cen[:, s * tile:(s + 1) * tile] * inv
                a_s[rows, cols] = (norm * ln_row(s, l, 0) + ln_row(s, l, 1)).astype(BF16)
                m_s[rows, cols] = (norm * ln_row(s, l, 2) + ln_row(s, l, 3)).astype(BF16)
                acc[rows, cols] = v[:, s * tile:(s + 1) * tile] + (row(s, l, 3) + row(s, l, 4 + rps))
            return carry

        lax.fori_loop(first, last, body, 0)

    def dot(lhs, slot, to):
        return jnp.dot(lhs, wbuf[slot, to], preferred_element_type=F32)

    def rotate(v, rows):
        u = v[:, :wide].astype(F32)
        turned = (u * tabs[0, rows, :] + pltpu.roll(u, wide - rot_half, 1) * tabs[1, rows, :]
                  + pltpu.roll(u, rot_half, 1) * tabs[2, rows, :])
        return turned.astype(BF16)

    def project(l, h, slot, i, ref):
        for rows in dot_blocks:
            v = (dot(a_s[rows, :], slot, i) + row(h, l, i)).astype(BF16)
            if i < 2:
                ref[rows, pl.ds(0, wide)] = rotate(v, rows)
                ref[rows, pl.ds(wide, tile - wide)] = v[:, wide:]
            else:
                ref[rows, :] = v

    def attend(h, b):
        width = (b + 1) * ROWS
        s = lax.dot_general(q_s[rows_of(b), :], k_s[pl.ds(0, width), :], (((1,), (1,)), ((), ())),
                            preferred_element_type=F32) * scale
        col = lax.broadcasted_iota(jnp.int32, (ROWS, width), 1)
        at = lax.broadcasted_iota(jnp.int32, (ROWS, width), 0) + b * ROWS
        s = jnp.where((col <= at) & (col < lens[0]), s, -1e30)
        e = jnp.exp(s - jnp.max(s, axis=-1, keepdims=True))
        p = (e * (1.0 / jnp.sum(e, axis=-1, keepdims=True))).astype(BF16)
        ctx[rows_of(b), cols_of(h)] = jnp.dot(p, v_s[pl.ds(0, width), :], preferred_element_type=F32).astype(BF16)

    def up(l, u, slot, to):
        s, rp = u % n, u // n
        for rows in dot_blocks:
            v = dot(m_s[rows, :], slot, to) + row(s, l, 4 + rp)
            g = (0.5 * v) * (1.0 + lax.erf(v * (0.5 ** 0.5)))
            act[rp, rows, cols_of(s)] = g.astype(BF16)

    def add_to(j, slot, to, lhs):
        for rows in dot_blocks:
            acc[rows, cols_of(j)] += dot(lhs(rows), slot, to)

    def down(v, slot, to):
        add_to(v % n_c, slot, to, lambda rows: act[v // n_c, rows, :])

    def head_step(l, h):
        k = l * per_layer + n_b + h
        slot = k % 2
        part0(k + 4)
        loaded(slot, 0)
        loaded(slot, 1)
        project(l, h, slot, 0, q_s)
        project(l, h, slot, 1, k_s)
        part1(k + 4)
        loaded(slot, 2)
        project(l, h, slot, 2, v_s)
        for b in range(blocks // 2):
            attend(h, b)
        part2(k + 4)
        for b in range(blocks // 2, blocks):
            attend(h, b)

        @pl.when(h == n_a - 1)
        def _():
            out_now(0, 1 - slot)

    def up_step(l, j):
        k = l * per_layer + j
        slot = k % 2

        @pl.when((l == 0) | (j > 0))
        def _():
            part0(k + 4)

        loaded(slot, 0)
        up(l, 2 * j, slot, 0)
        part1(k + 4)
        loaded(slot, 2)
        up(l, 2 * j + 1, slot, 2)
        part2(k + 4)

        @pl.when(j >= LATE)
        def _():
            loaded(slot, 3)
            down(j - LATE, slot, 3)

    def out_now(j, slot):
        loaded(slot, 1)
        add_to(j, slot, 1, lambda rows: ctx[rows, :])

    def down_now(j, slot, i):
        loaded(slot, i)
        down(n_b + 2 * j + i // 2, slot, i)

    def down_step(l, j):
        k = l * per_layer + n_a + n_b + j
        slot = k % 2
        part0(k + 4)

        @pl.when(j == 0)
        def _():
            down_now(j, slot, mine)

        @pl.when(j < n_c - 1)
        def _():
            out_now(j + 1, 1 - slot)

        part1(k + 4)

        @pl.when(j < n_c - 1)
        def _():
            down_now(j + 1, 1 - slot, mine)

        @pl.when(j < LATE)
        def _():
            loaded(slot, 3)
            down(n_b - LATE + j, slot, 3)

        part2(k + 4)
        down_now(j, slot, other)

        @pl.when(j >= n_c // 2)
        def _():
            cols = pl.ds(pl.multiple_of((2 * j - n_c) * tile, 2 * tile), 2 * tile)
            for b in range(blocks):
                xs[rows_of(b), cols] = acc[rows_of(b), cols].astype(BF16)

    def rotary_tables():
        freq = rope_row(2 * rot_half, wide)
        for b in range(blocks):
            at = (lax.broadcasted_iota(jnp.int32, (ROWS, wide), 0) + b * ROWS).astype(F32)
            lane = lax.broadcasted_iota(jnp.int32, (ROWS, wide), 1)
            angle = at * freq
            cos, sin = jnp.cos(angle), jnp.sin(angle)
            tabs[0, rows_of(b), :] = jnp.where(lane < 2 * rot_half, cos, 1.0)
            tabs[1, rows_of(b), :] = jnp.where(lane < rot_half, -sin, 0.0)
            tabs[2, rows_of(b), :] = jnp.where((lane >= rot_half) & (lane < 2 * rot_half), sin, 0.0)

    raw_rows = raw.shape[1]
    per_raw = tile * heads // raw_rows
    raws = num_layers * per_raw

    def get_raw(b):
        return pltpu.make_async_copy(
            wq_raw.at[b // per_raw, pl.ds(pl.multiple_of((b % per_raw) * raw_rows, raw_rows), raw_rows)],
            raw.at[b % 2], raw_in.at[b % 2])

    def put_raw(b):
        some = raw_rows // heads
        return pltpu.make_async_copy(
            turned.at[b % 2], wq.at[b // per_raw, :, pl.ds(pl.multiple_of((b % per_raw) * some, some), some)],
            raw_out.at[b % 2])

    def by_head(first, last):
        def body(b, carry):
            get_raw(b).wait()
            for q in range(raw.shape[2] // wide):
                raw32[pl.ds(q * raw_rows, raw_rows), :] = raw[b % 2, :, pl.ds(q * wide, wide)].astype(F32)

            @pl.when(b + 2 < raws)
            def _():
                get_raw(b + 2).start()

            @pl.when(b >= 2)
            def _():
                put_raw(b - 2).wait()

            for h in range(heads):
                for q in range(raw.shape[2] // wide):
                    turned[b % 2, h, :, pl.ds(q * wide, wide)] = (
                        raw32[pl.ds(q * raw_rows + h, raw_rows // heads, stride=heads), :].astype(BF16))
            put_raw(b).start()
            return carry

        lax.fori_loop(first, last, body, 0)

    def unpack_biases():
        for s in range(n):
            for g, at, count in ((bq_g, 0, 3), (bo_g, 3, 1), (bu_g, 4, rps), (bd_g, 4 + rps, 1)):
                for i in range(count):
                    v = g[s, :, pl.ds(i * tile, tile)].astype(F32)
                    for l in range(num_layers):
                        bias[s, l, pl.ds(at + i, 1), :] = v[l:l + 1]

    get_hidden = pltpu.make_async_copy(hid, xs, io_sem)
    get_hidden.start()
    get_raw(0).start()
    get_raw(1).start()
    barrier = pltpu.get_barrier_semaphore()
    for step in range(1, n):
        pl.semaphore_signal(barrier, inc=1, device_id={"fsdp": (f + step) % n}, device_id_type=MESH)
    pl.semaphore_signal(barrier, inc=1, device_id=to_mate, device_id_type=MESH)
    pl.semaphore_wait(barrier, n)

    smalls = ((ln_own, ln_g), (bq_own, bq_g), (bo_own, bo_g), (bu_own, bu_g), (bd_own, bd_g))
    own_first(0)
    for i, (own, everyone) in enumerate(smalls):
        for step in range(1, n):
            remote(own, everyone.at[f], small_send.at[i], small_recv.at[i], {"fsdp": (f + step) % n}).start()
    own_second(0)
    mine_too = [pltpu.make_async_copy(own, everyone.at[f], small_own.at[i]) for i, (own, everyone) in enumerate(smalls)]
    mine_too.append(pltpu.make_async_copy(lens_own, lens, small_own.at[len(smalls)]))
    for copy in mine_too:
        copy.start()
    rotary_tables()
    own_first(jnp.int32(1))
    left_mine(0)
    right_mine(0)
    for i, (own, everyone) in enumerate(smalls):
        ref = everyone.at[pl.ds(0, n - 1)]
        pltpu.make_async_copy(ref, ref, small_send.at[i]).wait()
        pltpu.make_async_copy(ref, ref, small_recv.at[i]).wait()
    for copy in mine_too:
        copy.wait()
    unpack_biases()
    own_second(jnp.int32(1))
    right_one(0)
    left_one(0)
    get_hidden.wait()
    norms = seq // norm_rows
    for i, part in enumerate((part0, part1, part2, part0)):
        layer_norms(0, norms * i // 4, norms * (i + 1) // 4)
        part(jnp.int32(2 + i // 3))
    by_head(0, raws // 3)
    part1(jnp.int32(3))
    by_head(raws // 3, raws * 2 // 3)
    part2(jnp.int32(3))
    by_head(raws * 2 // 3, raws)
    put_raw(raws - 2).wait()
    put_raw(raws - 1).wait()

    def layer(l, carry):
        def loop(count, step):
            def body(i, inner):
                step(l, i)
                return inner

            lax.fori_loop(0, count, body, 0)

        @pl.when(l > 0)
        def _():
            layer_norms(l, 0, norms // 2)
            part0(l * per_layer + 4)
            layer_norms(l, norms // 2, norms)

        loop(n_b, up_step)
        loop(n_a, head_step)
        loop(n_c, down_step)
        return carry

    lax.fori_loop(0, num_layers, layer, 0)
    for k in range(chunks - 3, chunks):
        wait_sent(k)


def solution(mesh):
    row_spec = P(("dp", "fsdp"), None, None)
    in_specs = (row_spec, P(("dp", "fsdp")), P(None, None, "fsdp"), P(None, "fsdp", None, None), P(None, "fsdp"),
                P(None, "fsdp", None), P(None, "fsdp"), P(None, "fsdp", None), P(None, "fsdp"), P(None, "fsdp", None),
                P(None, "fsdp"))
    n = mesh.shape["fsdp"]
    assert n % 2 == 0 and mesh.shape["dp"] % 2 == 0

    def local_step(hidden, lens, ln_par, w_qkv, b_qkv, w_out, b_out, w_up, b_up, w_down, b_down):
        _, seq, d_model = hidden.shape
        num_layers, tile, heads, triple = w_qkv.shape
        rps = w_down.shape[1] // tile
        assert hidden.shape[0] == 1 and n == 8 and n * tile == d_model and triple == 3 * tile and heads == n
        assert n * rps // 2 + 2 * (d_model // tile) == n * rps
        rot_half = tile // 8
        wide = 128
        raw_rows = 32 * heads
        dims = (n, num_layers, heads, tile, seq, d_model, rps, rot_half)
        chunks = num_layers * (heads + n * rps // 2 + d_model // tile)
        ring = n // 2
        vmem = pl.BlockSpec(memory_space=pltpu.VMEM)
        anywhere = pl.BlockSpec(memory_space=pl.ANY)
        dma = pltpu.SemaphoreType.DMA
        smalls = (ln_par, b_qkv, b_out, b_up, b_down)
        out, _, _ = pl.pallas_call(
            functools.partial(kernel, dims),
            name="layers",
            out_shape=(pltpu.VMEM((seq, d_model), BF16),
                       jax.ShapeDtypeStruct((chunks, 3, n, tile, tile), BF16),
                       jax.ShapeDtypeStruct((num_layers, heads, tile, triple), BF16)),
            in_specs=[anywhere] + [pl.BlockSpec(memory_space=pltpu.HBM)] * 6 + [anywhere] * 4,
            out_specs=(vmem, anywhere, anywhere),
            scratch_shapes=[
                pltpu.VMEM((seq, d_model), BF16),
                pltpu.VMEM((seq, d_model), BF16),
                pltpu.VMEM((seq, d_model), BF16),
                pltpu.VMEM((rps, seq, d_model), BF16),
                pltpu.VMEM((seq, d_model), F32),
                pltpu.VMEM((seq, tile), BF16),
                pltpu.VMEM((seq, tile), BF16),
                pltpu.VMEM((seq, tile), BF16),
                pltpu.VMEM((2, 4, d_model, tile), BF16),
                pltpu.VMEM((3, seq, wide), F32),
                pltpu.SMEM(lens.shape, lens.dtype),
                *[pltpu.VMEM((n,) + p.shape, p.dtype) for p in smalls],
                pltpu.VMEM((n, num_layers, 16, tile), F32),
                pltpu.VMEM((2, raw_rows, triple), BF16),
                pltpu.VMEM((raw_rows * triple // wide, wide), F32),
                pltpu.VMEM((2, heads, raw_rows // heads, triple), BF16),
                dma((SLOTS,)),
                dma((SLOTS, 3)),
                dma((SLOTS, 3)),
                dma((SLOTS, 3)),
                dma((SLOTS, 3)),
                dma((2, 4)),
                dma((5,)),
                dma((5,)),
                dma((6,)),
                dma((2,)),
                dma((2,)),
                dma,
            ],
            compiler_params=pltpu.CompilerParams(
                collective_id=0, has_side_effects=True, vmem_limit_bytes=59 * 2**20),
        )(hidden.reshape(seq, d_model), lens, *smalls,
          w_qkv.reshape(num_layers, tile * heads, triple), w_out, w_up, w_down)
        return out.reshape(1, seq, d_model)

    return jax.shard_map(local_step, mesh=mesh, in_specs=in_specs, out_specs=row_spec, check_vma=False)
```

```python
import functools

import jax
import jax.numpy as jnp
import numpy as np
from jax import lax
from jax.experimental import pallas as pl
from jax.experimental.pallas import tpu as pltpu
from jax.sharding import PartitionSpec as P

ROPE_BASE = 10000.0
LN_EPS = 1e-5
MESH = pl.DeviceIdType.MESH
SLOTS = 16
LATE = 4
ROWS = 256
DOT_ROWS = 256
F32 = jnp.float32
BF16 = jnp.bfloat16


def rope_row(rot_dim, width):
    inv_freq = np.float32(1.0) / (np.float32(ROPE_BASE) ** (np.arange(0, rot_dim, 2, dtype=np.float32) / np.float32(rot_dim)))
    lane = lax.broadcasted_iota(jnp.int32, (1, width), 1)
    row = jnp.zeros((1, width), F32)
    for i, value in enumerate(inv_freq):
        row = jnp.where((lane == i) | (lane == i + rot_dim // 2), float(value), row)
    return row


def kernel(dims, hid, lens_own, ln_own, bq_own, bo_own, bu_own, bd_own, wq_raw, wo, wu, wd, xs, gath, wq, a_s, m_s, ctx,
           act, acc, q_s, k_s, v_s, wbuf, tabs, lens, ln_g, bq_g, bo_g, bu_g, bd_g, bias, raw, raw32, turned, send, rs, ls, ysem, dd,
           ld, small_send, small_recv, small_own, from_l, from_r, raw_in, raw_out, io_sem):
    n, num_layers, heads, tile, seq, d_model, rps, rot_half = dims
    ring = n // 2
    n_a, n_b, n_c = heads, n * rps // 2, d_model // tile
    per_layer = n_a + n_b + n_c
    chunks = num_layers * per_layer
    wide = tabs.shape[2]
    scale = float(tile) ** -0.5

    d, f = lax.axis_index("dp"), lax.axis_index("fsdp")
    x, c = f // 2, f % 2
    par = d % 2
    right = ((x + 1) % ring) * 2 + c
    left = ((x + ring - 1) % ring) * 2 + c
    far = ((x + 2) % ring) * 2 + c
    sib = x * 2 + 1 - c
    mate = d + 1 - 2 * par
    mine, other = 2 * par, 2 - 2 * par

    def remote(src, dst, s_sem, r_sem, where):
        return pltpu.make_async_remote_copy(
            src_ref=src, dst_ref=dst, send_sem=s_sem, recv_sem=r_sem, device_id=where, device_id_type=MESH)

    halves = [pl.ds(i * (tile // 2), tile // 2) for i in range(2)]
    to_right, to_left, to_sib, to_mate = {"fsdp": right}, {"fsdp": left}, {"fsdp": sib}, {"dp": mate}

    def q_tile(l, h, i):
        return wq.at[l, h, :, pl.ds(i * tile, tile) if isinstance(i, int) else pl.ds(pl.multiple_of(i * tile, tile), tile)]

    def up_tile(l, u):
        return wu.at[l, :, pl.ds(pl.multiple_of((u % n) * (rps * tile) + (u // n) * tile, tile), tile)]

    def down_tile(l, v):
        return wd.at[l, pl.ds(pl.multiple_of((v // n_c) * tile, tile), tile),
                     pl.ds(pl.multiple_of((v % n_c) * tile, tile), tile)]

    def out_tile(l, j):
        return wo.at[l, :, pl.ds(pl.multiple_of(j * tile, tile), tile)]

    def with_own(k, go):
        l, r = k // per_layer, k % per_layer

        @pl.when(r < n_b)
        def _():
            go(lambda i: down_tile(l, r) if isinstance(i, int) and i == 1 else up_tile(l, 2 * r + i // 2))

        @pl.when((r >= n_b) & (r < n_b + n_a))
        def _():
            go(lambda i: q_tile(l, r - n_b, i))

        @pl.when(r >= n_a + n_b)
        def _():
            j = r - n_a - n_b
            go(lambda i: out_tile(l, j) if isinstance(i, int) and i == 1 else down_tile(l, n_b + 2 * j + i // 2))

    def own_first(k):
        slot = k % SLOTS
        at_once = isinstance(k, int)

        def go(own):
            if at_once:
                for half, part in enumerate(halves):
                    src, dst = own(mine).at[part], gath.at[k, mine, f].at[part]
                    remote(src, dst, send.at[slot], from_l.at[half], to_right).start()
                    remote(src, dst, send.at[slot], from_r.at[half], to_left).start()
            else:
                remote(own(mine), gath.at[k, mine, f], send.at[slot], rs.at[slot, 0], to_right).start()
                remote(own(1), gath.at[k, 1, f], send.at[slot], ls.at[slot, 0], to_left).start()
            for role, i in enumerate((mine, 1)):
                remote(own(i), gath.at[k, i, f], send.at[slot], dd.at[slot, role], to_sib).start()

        with_own(k, go)

    def own_second(k):
        slot = k % SLOTS
        at_once = isinstance(k, int)

        def go(own):
            remote(own(1), gath.at[k, 1, f], send.at[slot], rs.at[slot, 1], to_right).start()
            if at_once:
                remote(own(1), gath.at[k, 1, f], send.at[slot], ls.at[slot, 0], to_left).start()
            else:
                remote(own(mine), gath.at[k, mine, f], send.at[slot], ls.at[slot, 1], to_left).start()
            remote(own(other), gath.at[k, other, f], send.at[slot], dd.at[slot, 2], to_sib).start()

        with_own(k, go)

    def wait_tile(sem):
        ref = gath.at[0, 0, 0]
        pltpu.make_async_copy(ref, ref, sem).wait()

    def pass_on(k, i, s, sem, where):
        t = gath.at[k, i, s]
        remote(t, t, send.at[k % SLOTS], sem, where).start()

    def both_mine(k):
        slot = k % SLOTS
        for half, part in enumerate(halves):
            for sem, s, onward, i in ((from_l, left, True, 0), (from_r, right, False, 1)):
                t = gath.at[k, mine, s].at[part]
                pltpu.make_async_copy(t, t, sem.at[half]).wait()
                remote(t, t, send.at[slot], ysem.at[slot, i], to_mate).start()
                if onward:
                    remote(t, t, send.at[slot], rs.at[slot, 2], to_right).start()
                remote(t, t, send.at[slot], dd.at[slot, 0], to_sib).start()

    def left_mine(k):
        slot = k % SLOTS
        wait_tile(rs.at[slot, 0])
        pass_on(k, mine, left, rs.at[slot, 2], to_right)
        pass_on(k, mine, left, ysem.at[slot, 0], to_mate)
        pass_on(k, mine, left, dd.at[slot, 0], to_sib)

    def right_one(k):
        slot = k % SLOTS
        wait_tile(ls.at[slot, 0])
        pass_on(k, 1, right, ls.at[slot, 2], to_left)
        pass_on(k, 1, right, dd.at[slot, 1], to_sib)

    def right_mine(k):
        slot = k % SLOTS
        wait_tile(ls.at[slot, 1])
        pass_on(k, mine, right, ysem.at[slot, 1], to_mate)
        pass_on(k, mine, right, dd.at[slot, 0], to_sib)

    def left_one(k):
        slot = k % SLOTS
        wait_tile(rs.at[slot, 1])
        pass_on(k, 1, left, dd.at[slot, 1], to_sib)

    def from_sides(k):
        left_mine(k)
        right_one(k)

    def from_sides_again(k):
        right_mine(k)
        left_one(k)

    def from_far(k):
        slot = k % SLOTS
        wait_tile(rs.at[slot, 2])
        pass_on(k, mine, far, ysem.at[slot, 2], to_mate)
        pass_on(k, mine, far, dd.at[slot, 0], to_sib)
        wait_tile(ls.at[slot, 2])
        pass_on(k, 1, far, dd.at[slot, 1], to_sib)

    def from_mate(i, s):
        def do(k):
            slot = k % SLOTS
            wait_tile(ysem.at[slot, i])
            pass_on(k, other, s, dd.at[slot, 2], to_sib)

        return do

    sent_tiles = 3 * (ring - 1) + 3 * ring

    def wait_sib(k, role):
        ref = gath.at[0, 0, pl.ds(0, ring)]
        pltpu.make_async_copy(ref, ref, dd.at[k % SLOTS, role]).wait()

    def wait_sent(k):
        ref = gath.at[0, :, pl.ds(0, sent_tiles // 3)]
        pltpu.make_async_copy(ref, ref, send.at[k % SLOTS]).wait()

    def load_tile(k, kk, i, to, own):
        slot = k % 2
        for step in range(1, n):
            s = (f + step) % n
            pltpu.make_async_copy(
                gath.at[kk, i, s], wbuf.at[slot, to, pl.ds(pl.multiple_of(s * tile, tile), tile)], ld.at[slot, to]).start()
        pltpu.make_async_copy(own, wbuf.at[slot, to, pl.ds(pl.multiple_of(f * tile, tile), tile)], ld.at[slot, to]).start()

    def load_down(k, i):
        j = k % per_layer - n_a - n_b
        load_tile(k, k, i, i, down_tile(k // per_layer, n_b + 2 * j + i // 2))

    def load(k):
        l, r = k // per_layer, k % per_layer
        for role in range(3):
            wait_sib(k, role)

        @pl.when(r < n_b)
        def _():
            for i in (0, 2):
                load_tile(k, k, i, i, up_tile(l, 2 * r + i // 2))

        @pl.when((r >= LATE) & (r < n_b))
        def _():
            load_tile(k, k - LATE, 1, 3, down_tile(l, r - LATE))

        @pl.when(r >= n_b)
        def _():
            for i in range(3):
                load_tile(k, k, i, i, q_tile(l, r - n_b, i))

    def load_first(k):
        l, j = k // per_layer, k % per_layer - n_a - n_b
        for role in range(2):
            wait_sib(k, role)
        load_tile(k, k, 1, 1, out_tile(l, j))
        load_down(k, mine)

        @pl.when(j < LATE)
        def _():
            load_tile(k, k - n_a - LATE, 1, 3, down_tile(l, n_b - LATE + j))

    def load_last(k):
        wait_sib(k, 2)
        load_down(k, other)

    def loaded(slot, to):
        pltpu.make_async_copy(wbuf.at[slot, to], wbuf.at[slot, to], ld.at[slot, to]).wait()

    def within(k, do, phases=None):
        r = k % per_layer
        these = {None: True, "first": r < n_a + n_b, "last": r >= n_a + n_b}[phases]

        @pl.when((k >= 0) & (k < chunks) & these)
        def _():
            do(k)

    def part0(t):
        within(t - 7, wait_sent)
        within(t, own_first)
        within(t - 1, from_sides)
        within(t - 4, from_mate(2, far), "last")

    def part1(t):
        within(t - 2, from_far)
        within(t - 3, from_mate(1, right))
        within(t - 3, from_mate(2, far), "first")
        within(t - 4, load_last, "last")

    def part2(t):
        within(t, own_second)
        within(t - 1, from_sides_again)
        within(t - 2, from_mate(0, left))
        within(t - 2, load_first, "last")
        within(t - 3, load, "first")

    blocks = seq // ROWS

    def rows_of(b):
        return pl.ds(b * ROWS, ROWS)

    dot_blocks = [pl.ds(b * DOT_ROWS, DOT_ROWS) for b in range(seq // DOT_ROWS)]

    def cols_of(j):
        return pl.ds(pl.multiple_of(j * tile, tile), tile)

    def row(s, l, i):
        return bias[s, l, pl.ds(i, 1), :]

    def ln_row(s, l, i):
        return ln_g[s, l, pl.ds(i, 1), :]

    norm_rows = 128

    def layer_norms(l, first, last):
        step = norm_rows

        def body(b, carry):
            rows = pl.ds(pl.multiple_of(b * step, step), step)
            v = xs[rows, :].astype(F32)
            cen = v - jnp.mean(v, axis=-1, keepdims=True)
            inv = lax.rsqrt(jnp.mean(cen * cen, axis=-1, keepdims=True) + LN_EPS)
            for s in range(n):
                cols = pl.ds(s * tile, tile)
                norm = cen[:, s * tile:(s + 1) * tile] * inv
                a_s[rows, cols] = (norm * ln_row(s, l, 0) + ln_row(s, l, 1)).astype(BF16)
                m_s[rows, cols] = (norm * ln_row(s, l, 2) + ln_row(s, l, 3)).astype(BF16)
                acc[rows, cols] = v[:, s * tile:(s + 1) * tile] + (row(s, l, 3) + row(s, l, 4 + rps))
            return carry

        lax.fori_loop(first, last, body, 0)

    def dot(lhs, slot, to):
        return jnp.dot(lhs, wbuf[slot, to], preferred_element_type=F32)

    def rotate(v, rows):
        u = v[:, :wide].astype(F32)
        turned = (u * tabs[0, rows, :] + pltpu.roll(u, wide - rot_half, 1) * tabs[1, rows, :]
                  + pltpu.roll(u, rot_half, 1) * tabs[2, rows, :])
        return turned.astype(BF16)

    def project(l, h, slot, i, ref):
        for rows in dot_blocks:
            v = (dot(a_s[rows, :], slot, i) + row(h, l, i)).astype(BF16)
            if i < 2:
                ref[rows, pl.ds(0, wide)] = rotate(v, rows)
                ref[rows, pl.ds(wide, tile - wide)] = v[:, wide:]
            else:
                ref[rows, :] = v

    def attend(h, b):
        width = (b + 1) * ROWS
        s = lax.dot_general(q_s[rows_of(b), :], k_s[pl.ds(0, width), :], (((1,), (1,)), ((), ())),
                            preferred_element_type=F32) * scale
        col = lax.broadcasted_iota(jnp.int32, (ROWS, width), 1)
        at = lax.broadcasted_iota(jnp.int32, (ROWS, width), 0) + b * ROWS
        s = jnp.where((col <= at) & (col < lens[0]), s, -1e30)
        e = jnp.exp(s - jnp.max(s, axis=-1, keepdims=True))
        p = (e * (1.0 / jnp.sum(e, axis=-1, keepdims=True))).astype(BF16)
        ctx[rows_of(b), cols_of(h)] = jnp.dot(p, v_s[pl.ds(0, width), :], preferred_element_type=F32).astype(BF16)

    def up(l, u, slot, to):
        s, rp = u % n, u // n
        for rows in dot_blocks:
            v = dot(m_s[rows, :], slot, to) + row(s, l, 4 + rp)
            g = (0.5 * v) * (1.0 + lax.erf(v * (0.5 ** 0.5)))
            act[rp, rows, cols_of(s)] = g.astype(BF16)

    def add_to(j, slot, to, lhs):
        for rows in dot_blocks:
            acc[rows, cols_of(j)] += dot(lhs(rows), slot, to)

    def down(v, slot, to):
        add_to(v % n_c, slot, to, lambda rows: act[v // n_c, rows, :])

    def head_step(l, h):
        k = l * per_layer + n_b + h
        slot = k % 2
        part0(k + 4)
        loaded(slot, 0)
        loaded(slot, 1)
        project(l, h, slot, 0, q_s)
        project(l, h, slot, 1, k_s)
        part1(k + 4)
        loaded(slot, 2)
        project(l, h, slot, 2, v_s)
        for b in range(blocks // 2):
            attend(h, b)
        part2(k + 4)
        for b in range(blocks // 2, blocks):
            attend(h, b)

        @pl.when(h == n_a - 1)
        def _():
            out_now(0, 1 - slot)

    def up_step(l, j):
        k = l * per_layer + j
        slot = k % 2

        @pl.when((l == 0) | (j > 0))
        def _():
            part0(k + 4)

        loaded(slot, 0)
        up(l, 2 * j, slot, 0)
        part1(k + 4)
        loaded(slot, 2)
        up(l, 2 * j + 1, slot, 2)
        part2(k + 4)

        @pl.when(j >= LATE)
        def _():
            loaded(slot, 3)
            down(j - LATE, slot, 3)

    def out_now(j, slot):
        loaded(slot, 1)
        add_to(j, slot, 1, lambda rows: ctx[rows, :])

    def down_now(j, slot, i):
        loaded(slot, i)
        down(n_b + 2 * j + i // 2, slot, i)

    def down_step(l, j):
        k = l * per_layer + n_a + n_b + j
        slot = k % 2
        part0(k + 4)

        @pl.when(j == 0)
        def _():
            down_now(j, slot, mine)

        @pl.when(j < n_c - 1)
        def _():
            out_now(j + 1, 1 - slot)

        part1(k + 4)

        @pl.when(j < n_c - 1)
        def _():
            down_now(j + 1, 1 - slot, mine)

        @pl.when(j < LATE)
        def _():
            loaded(slot, 3)
            down(n_b - LATE + j, slot, 3)

        part2(k + 4)
        down_now(j, slot, other)

        @pl.when(j >= n_c // 2)
        def _():
            cols = pl.ds(pl.multiple_of((2 * j - n_c) * tile, 2 * tile), 2 * tile)
            for b in range(blocks):
                xs[rows_of(b), cols] = acc[rows_of(b), cols].astype(BF16)

    def rotary_tables():
        freq = rope_row(2 * rot_half, wide)
        for b in range(blocks):
            at = (lax.broadcasted_iota(jnp.int32, (ROWS, wide), 0) + b * ROWS).astype(F32)
            lane = lax.broadcasted_iota(jnp.int32, (ROWS, wide), 1)
            angle = at * freq
            cos, sin = jnp.cos(angle), jnp.sin(angle)
            tabs[0, rows_of(b), :] = jnp.where(lane < 2 * rot_half, cos, 1.0)
            tabs[1, rows_of(b), :] = jnp.where(lane < rot_half, -sin, 0.0)
            tabs[2, rows_of(b), :] = jnp.where((lane >= rot_half) & (lane < 2 * rot_half), sin, 0.0)

    raw_rows = raw.shape[1]
    per_raw = tile * heads // raw_rows
    raws = num_layers * per_raw

    def get_raw(b):
        return pltpu.make_async_copy(
            wq_raw.at[b // per_raw, pl.ds(pl.multiple_of((b % per_raw) * raw_rows, raw_rows), raw_rows)],
            raw.at[b % 2], raw_in.at[b % 2])

    def put_raw(b):
        some = raw_rows // heads
        return pltpu.make_async_copy(
            turned.at[b % 2], wq.at[b // per_raw, :, pl.ds(pl.multiple_of((b % per_raw) * some, some), some)],
            raw_out.at[b % 2])

    def by_head(first, last):
        def body(b, carry):
            get_raw(b).wait()
            for q in range(raw.shape[2] // wide):
                raw32[pl.ds(q * raw_rows, raw_rows), :] = raw[b % 2, :, pl.ds(q * wide, wide)].astype(F32)

            @pl.when(b + 2 < raws)
            def _():
                get_raw(b + 2).start()

            @pl.when(b >= 2)
            def _():
                put_raw(b - 2).wait()

            for h in range(heads):
                for q in range(raw.shape[2] // wide):
                    turned[b % 2, h, :, pl.ds(q * wide, wide)] = (
                        raw32[pl.ds(q * raw_rows + h, raw_rows // heads, stride=heads), :].astype(BF16))
            put_raw(b).start()
            return carry

        lax.fori_loop(first, last, body, 0)

    def unpack_biases():
        for s in range(n):
            for g, at, count in ((bq_g, 0, 3), (bo_g, 3, 1), (bu_g, 4, rps), (bd_g, 4 + rps, 1)):
                for i in range(count):
                    v = g[s, :, pl.ds(i * tile, tile)].astype(F32)
                    for l in range(num_layers):
                        bias[s, l, pl.ds(at + i, 1), :] = v[l:l + 1]

    get_hidden = pltpu.make_async_copy(hid, xs, io_sem)
    get_hidden.start()
    get_raw(0).start()
    get_raw(1).start()
    barrier = pltpu.get_barrier_semaphore()
    for step in range(1, n):
        pl.semaphore_signal(barrier, inc=1, device_id={"fsdp": (f + step) % n}, device_id_type=MESH)
    pl.semaphore_signal(barrier, inc=1, device_id=to_mate, device_id_type=MESH)
    pl.semaphore_wait(barrier, n)

    smalls = ((ln_own, ln_g), (bq_own, bq_g), (bo_own, bo_g), (bu_own, bu_g), (bd_own, bd_g))
    own_first(0)
    for i, (own, everyone) in enumerate(smalls):
        for step in range(1, n):
            remote(own, everyone.at[f], small_send.at[i], small_recv.at[i], {"fsdp": (f + step) % n}).start()
    own_second(0)
    mine_too = [pltpu.make_async_copy(own, everyone.at[f], small_own.at[i]) for i, (own, everyone) in enumerate(smalls)]
    mine_too.append(pltpu.make_async_copy(lens_own, lens, small_own.at[len(smalls)]))
    for copy in mine_too:
        copy.start()
    rotary_tables()
    own_first(jnp.int32(1))
    both_mine(0)
    for i, (own, everyone) in enumerate(smalls):
        ref = everyone.at[pl.ds(0, n - 1)]
        pltpu.make_async_copy(ref, ref, small_send.at[i]).wait()
        pltpu.make_async_copy(ref, ref, small_recv.at[i]).wait()
    for copy in mine_too:
        copy.wait()
    unpack_biases()
    own_second(jnp.int32(1))
    right_one(0)
    left_one(0)
    get_hidden.wait()
    norms = seq // norm_rows
    for i, part in enumerate((part0, part1, part2, part0)):
        layer_norms(0, norms * i // 4, norms * (i + 1) // 4)
        part(jnp.int32(2 + i // 3))
    by_head(0, raws // 3)
    part1(jnp.int32(3))
    by_head(raws // 3, raws * 2 // 3)
    part2(jnp.int32(3))
    by_head(raws * 2 // 3, raws)
    put_raw(raws - 2).wait()
    put_raw(raws - 1).wait()

    def layer(l, carry):
        def loop(count, step):
            def body(i, inner):
                step(l, i)
                return inner

            lax.fori_loop(0, count, body, 0)

        @pl.when(l > 0)
        def _():
            layer_norms(l, 0, norms // 2)
            part0(l * per_layer + 4)
            layer_norms(l, norms // 2, norms)

        loop(n_b, up_step)
        loop(n_a, head_step)
        loop(n_c, down_step)
        return carry

    lax.fori_loop(0, num_layers, layer, 0)
    for k in range(chunks - 3, chunks):
        wait_sent(k)


def solution(mesh):
    row_spec = P(("dp", "fsdp"), None, None)
    in_specs = (row_spec, P(("dp", "fsdp")), P(None, None, "fsdp"), P(None, "fsdp", None, None), P(None, "fsdp"),
                P(None, "fsdp", None), P(None, "fsdp"), P(None, "fsdp", None), P(None, "fsdp"), P(None, "fsdp", None),
                P(None, "fsdp"))
    n = mesh.shape["fsdp"]
    assert n % 2 == 0 and mesh.shape["dp"] % 2 == 0

    def local_step(hidden, lens, ln_par, w_qkv, b_qkv, w_out, b_out, w_up, b_up, w_down, b_down):
        _, seq, d_model = hidden.shape
        num_layers, tile, heads, triple = w_qkv.shape
        rps = w_down.shape[1] // tile
        assert hidden.shape[0] == 1 and n == 8 and n * tile == d_model and triple == 3 * tile and heads == n
        assert n * rps // 2 + 2 * (d_model // tile) == n * rps
        rot_half = tile // 8
        wide = 128
        raw_rows = 32 * heads
        dims = (n, num_layers, heads, tile, seq, d_model, rps, rot_half)
        chunks = num_layers * (heads + n * rps // 2 + d_model // tile)
        ring = n // 2
        vmem = pl.BlockSpec(memory_space=pltpu.VMEM)
        anywhere = pl.BlockSpec(memory_space=pl.ANY)
        dma = pltpu.SemaphoreType.DMA
        smalls = (ln_par, b_qkv, b_out, b_up, b_down)
        out, _, _ = pl.pallas_call(
            functools.partial(kernel, dims),
            name="layers",
            out_shape=(pltpu.VMEM((seq, d_model), BF16),
                       jax.ShapeDtypeStruct((chunks, 3, n, tile, tile), BF16),
                       jax.ShapeDtypeStruct((num_layers, heads, tile, triple), BF16)),
            in_specs=[anywhere] + [pl.BlockSpec(memory_space=pltpu.HBM)] * 6 + [anywhere] * 4,
            out_specs=(vmem, anywhere, anywhere),
            scratch_shapes=[
                pltpu.VMEM((seq, d_model), BF16),
                pltpu.VMEM((seq, d_model), BF16),
                pltpu.VMEM((seq, d_model), BF16),
                pltpu.VMEM((rps, seq, d_model), BF16),
                pltpu.VMEM((seq, d_model), F32),
                pltpu.VMEM((seq, tile), BF16),
                pltpu.VMEM((seq, tile), BF16),
                pltpu.VMEM((seq, tile), BF16),
                pltpu.VMEM((2, 4, d_model, tile), BF16),
                pltpu.VMEM((3, seq, wide), F32),
                pltpu.SMEM(lens.shape, lens.dtype),
                *[pltpu.VMEM((n,) + p.shape, p.dtype) for p in smalls],
                pltpu.VMEM((n, num_layers, 16, tile), F32),
                pltpu.VMEM((2, raw_rows, triple), BF16),
                pltpu.VMEM((raw_rows * triple // wide, wide), F32),
                pltpu.VMEM((2, heads, raw_rows // heads, triple), BF16),
                dma((SLOTS,)),
                dma((SLOTS, 3)),
                dma((SLOTS, 3)),
                dma((SLOTS, 3)),
                dma((SLOTS, 3)),
                dma((2, 4)),
                dma((5,)),
                dma((5,)),
                dma((6,)),
                dma((2,)),
                dma((2,)),
                dma((2,)),
                dma((2,)),
                dma,
            ],
            compiler_params=pltpu.CompilerParams(
                collective_id=0, has_side_effects=True, vmem_limit_bytes=59 * 2**20),
        )(hidden.reshape(seq, d_model), lens, *smalls,
          w_qkv.reshape(num_layers, tile * heads, triple), w_out, w_up, w_down)
        return out.reshape(1, seq, d_model)

    return jax.shard_map(local_step, mesh=mesh, in_specs=in_specs, out_specs=row_spec, check_vma=False)
```
